256 devices in a mesh: row: 16 (over z, core), col: 16 (over y, x).
Axes of the slice: x: 4, y: 4, z: 8, core: 2. Of those that a mesh axis runs over, the one named last changes fastest.
Arguments:
- velocity: float32 [1, 3, 128, 256, 256], P(None, None, 'row', 'col'), may hold values from -6 to 6
- tendency: float32 [1, 3, 128, 256, 256], P(None, None, 'row', 'col'), may hold values from -6 to 6
- step_size: float32 [1], replicated, may hold values from 0.1 to 0.6
- lift_weight: float32 [32, 3], replicated, may hold values from -3.5 to 3.5
- lift_bias: float32 [32], replicated, may hold values from -3 to 3
- spectral_weight: bfloat16 [2, 32, 32, 32, 1024], P(None, 'row', 'col'), may hold values from -6 to 6
- local_weight: float32 [32, 32], replicated, may hold values from -1 to 1
- local_bias: float32 [32], replicated, may hold values from -3 to 3
Outputs:
- features: bfloat16 [1, 32, 128, 256, 256], P(None, None, 'row', 'col')
The draws below stay inside these ranges and needn't reach their ends.
All inputs are finite; a program needn't handle non-finite values.
Results may differ from the reference program's by a relative error of at most 0.001.
Values sent between devices are 32-bit elements; how exact they have to be, the bound alone decides.
A program may use at most 64 MiB of HBM per device.

```python
import math
import jax
import jax.numpy as jnp
from jax import lax

CHANNELS = 32
KX = 32
KY = 32
KZ = 32
NZ = 256
SAMPLES = 1
NX = 128
NY = 256


def block_levels(key, dims, shards, low, high):
    factor_of, own = 1.0, jax.random.fold_in(key, 6)
    for position, shards_of in shards:
        heights = jnp.exp(jax.random.uniform(jax.random.fold_in(own, position), (shards_of,), jnp.float32, low / len(shards), high / len(shards)))
        factor_of = factor_of * jnp.repeat(heights, dims[position] // shards_of).reshape([-1 if axis == position else 1 for axis in range(len(dims))])
    return factor_of


def centred(key, dims, scale, reach, pieces=(), kind=jnp.bfloat16):
    gain = block_levels(key, dims, pieces, -0.22, 0.18) if pieces else 1.0
    entries = jax.random.normal(key, dims, jnp.float32) * scale * gain
    return jnp.minimum(jnp.maximum(entries, -reach), reach).astype(kind)


def setup_inputs(seed: int = 0) -> dict:
    arg_keys = jax.random.split(jax.random.key(seed), 9)
    velocity = centred(arg_keys[0], (SAMPLES, 3, NX, NY, NZ), 1.0, 6.0, ((2, 16), (3, 16)), jnp.float32)
    tendency = centred(arg_keys[1], (SAMPLES, 3, NX, NY, NZ), 1.0, 6.0, ((2, 16), (3, 16)), jnp.float32)
    step_size = jnp.clip(jnp.exp(jax.random.uniform(arg_keys[2], (SAMPLES,), jnp.float32, math.log(0.1), math.log(0.6))), 0.1, 0.6)
    lift_weight = centred(arg_keys[3], (CHANNELS, 3), 3 ** -0.5, 3.5, (), jnp.float32)
    lift_bias = centred(arg_keys[4], (CHANNELS,), 0.5, 3.0, (), jnp.float32)
    spectral_weight = centred(arg_keys[5], (2, KY, KZ, KX, CHANNELS * CHANNELS), 1.0, 6.0, ((1, 16), (2, 16)))
    local_weight = centred(arg_keys[6], (CHANNELS, CHANNELS), CHANNELS ** -0.5, 1.0, (), jnp.float32)
    local_bias = centred(arg_keys[7], (CHANNELS,), 0.5, 3.0, (), jnp.float32)
    return dict(velocity=velocity, tendency=tendency, step_size=step_size, lift_weight=lift_weight, lift_bias=lift_bias, spectral_weight=spectral_weight, local_weight=local_weight, local_bias=local_bias)


def positions(count, length):
    index = jnp.arange(count, dtype=jnp.int32)
    return jnp.where(index < count // 2, index, length - count + index).astype(jnp.int32)


def reference(velocity, tendency, step_size, lift_weight, lift_bias, spectral_weight, local_weight, local_bias):
    highest = lax.Precision.HIGHEST
    x_pos = positions(KX, NX)
    y_pos = positions(KY, NY)
    z_pos = jnp.arange(KZ, dtype=jnp.int32)
    volume = NX * NY * NZ
    weights = spectral_weight.astype(jnp.float32).reshape(2, KY, KZ, KX, CHANNELS, CHANNELS)
    complex_weights = weights[0] + 1j * weights[1]
    combined = jnp.dot(local_weight, lift_weight, precision=highest)
    offset = jnp.dot(local_weight, lift_bias, precision=highest) + local_bias
    results = []
    for sample in range(SAMPLES):
        advanced = velocity[sample] + step_size[sample] * tendency[sample]

        def forward(channel):
            lifted = (lift_weight[channel, 0] * advanced[0] + lift_weight[channel, 1] * advanced[1]
                      + lift_weight[channel, 2] * advanced[2] + lift_bias[channel])
            spectrum = jnp.fft.rfftn(lifted)
            kept = spectrum[x_pos][:, y_pos][:, :, :KZ]
            return kept / volume

        coeffs = lax.map(forward, jnp.arange(CHANNELS, dtype=jnp.int32))
        mixed = jnp.einsum("egaoi,iaeg->oaeg", complex_weights, coeffs, precision=highest)

        def inverse(channel):
            full = jnp.zeros((NX, NY, NZ // 2 + 1), mixed.dtype)
            full = full.at[x_pos[:, None, None], y_pos[None, :, None], z_pos[None, None, :]].set(mixed[channel])
            spectral = jnp.fft.irfftn(full, s=(NX, NY, NZ)) * volume
            local = (combined[channel, 0] * advanced[0] + combined[channel, 1] * advanced[1]
                     + combined[channel, 2] * advanced[2] + offset[channel])
            return jax.nn.gelu(spectral + local).astype(jnp.bfloat16)

        results.append(lax.map(inverse, jnp.arange(CHANNELS, dtype=jnp.int32)))
    return jnp.stack(results, 0)
```

```python
import functools
import math

import jax
import jax.numpy as jnp
import numpy as np
from jax import lax
from jax.experimental import pallas as pl
from jax.experimental.pallas import tpu as pltpu
from jax.sharding import PartitionSpec as P

F32 = jnp.float32
BF16 = jnp.bfloat16
MESH = pl.DeviceIdType.MESH
N = 16


def split(x):
    hi = x.astype(BF16)
    lo = (x - hi.astype(F32)).astype(BF16)
    return hi, lo


def dot(a, b):
    return jnp.dot(a, b, preferred_element_type=F32)


def dot_nt(a, b):
    return lax.dot_general(a, b, (((1,), (1,)), ((), ())), preferred_element_type=F32)


def np_split(x):
    x = np.asarray(x, np.float64)
    hi = x.astype(np.float32).astype(jnp.bfloat16)
    lo = (x - hi.astype(np.float64)).astype(np.float32).astype(jnp.bfloat16)
    return hi, lo


@functools.lru_cache(None)
def tables():
    turn = 2.0 * np.pi
    ix = np.arange
    waves = np.where(ix(32) < 16, ix(32), ix(32) - 32)
    eye8 = np.eye(8)
    z_angle = turn * (ix(32)[:, None] * ix(256)[None, :] % 256) / 256
    z_hi, z_lo = np_split(np.concatenate([np.cos(z_angle), -np.sin(z_angle)], 0))
    fwd_z = np.concatenate([z_hi, z_lo, z_hi], 1)
    a = turn * waves[None, :] * ix(16)[:, None] / 256
    by = np.zeros((2, 8, 16, 2, 32, 8))
    for x in range(8):
        by[0, x, :, 0, :, x] = np.cos(a)
        by[1, x, :, 0, :, x] = np.sin(a)
        by[0, x, :, 1, :, x] = -np.sin(a)
        by[1, x, :, 1, :, x] = np.cos(a)
    by_hi, by_lo = np_split(by.reshape(256, 512))
    b = turn * (waves[None, :] * ix(16)[:, None] % 16) / 16
    b = np.repeat(b, 8, axis=1)
    tw_y = np.stack([np.cos(b), np.sin(b)], 0).astype(np.float32)
    c = turn * waves[None, :] * ix(8)[:, None] / 128
    bx = []
    for quarter in (0.0, np.pi / 2):
        t = np.zeros((2, 8, 8, 8, 2, 32))
        for e in range(8):
            t[0, e, :, e, 0, :] = np.cos(c + quarter)
            t[1, e, :, e, 0, :] = np.sin(c + quarter)
            t[0, e, :, e, 1, :] = -np.sin(c + quarter)
            t[1, e, :, e, 1, :] = np.cos(c + quarter)
        bx.append(t.reshape(128, 512))
    bx = np.stack(bx, 0).astype(np.float32)
    d = turn * (waves[None, :] * ix(16)[:, None] % 16) / 16
    d = np.tile(d, (1, 16))
    tw_x = np.stack([np.cos(d), np.sin(d)], 0).astype(np.float32)
    sel = (ix(1024)[:, None] // 32 == ix(128)[None, :] // 4).astype(jnp.bfloat16)
    f = turn * (waves[None, :] * ix(128)[:, None] % 128) / 128
    ex_hi, ex_lo = np_split(np.concatenate([np.cos(f), np.sin(f)], 1))
    inv_x = np.concatenate([ex_hi, ex_hi, ex_lo], 1)
    g = turn * waves[:, None] * ix(32)[None, :] / 256
    ey = np.zeros((2, 32, 8, 2, 8, 16))
    for x in range(8):
        for blk in range(2):
            ey[0, :, x, blk, x, :] = np.cos(g[:, blk * 16:blk * 16 + 16])
            ey[1, :, x, blk, x, :] = -np.sin(g[:, blk * 16:blk * 16 + 16])
    ey_hi, ey_lo = np_split(ey.reshape(512, 256))
    h = turn * (waves[None, :] * ix(8)[:, None] % 8) / 8
    h = np.repeat(h, 8, axis=1)
    tw_i = np.stack([np.cos(h), np.sin(h)], 0).astype(np.float32)
    ez = np.zeros((16, 2, 2, 2, 2, 256))
    weight = np.where(ix(32) == 0, 1.0, 2.0)[:, None]
    cz = (weight * np.cos(z_angle)).reshape(16, 2, 256)
    sz = (-weight * np.sin(z_angle)).reshape(16, 2, 256)
    for o in range(2):
        ez[:, o, :, 0, o, :] = cz
        ez[:, o, :, 1, o, :] = sz
    ez_hi, ez_lo = np_split(ez.reshape(128, 512))
    inv_z = np.concatenate([ez_hi, ez_hi, ez_lo], 0)
    return dict(
        fwd_z=fwd_z, by=np.stack([by_hi, by_lo], 0), tw_y=tw_y, bx=bx, tw_x=tw_x, sel=sel,
        inv_x=inv_x, ey=np.stack([ey_hi, ey_lo], 0), tw_i=tw_i, inv_z=inv_z,
    )


def forward_z(advanced, fwd_z):
    hi, lo = split(advanced)
    return dot_nt(fwd_z, jnp.concatenate([hi, hi, lo], 1))


def forward_y(arrived, by_hi, by_lo, tw_c, tw_s):
    hi, lo = split(arrived)
    u = dot(jnp.concatenate([hi, lo], 0), by_hi)
    u = u[:128] + u[128:] + dot(hi, by_lo)
    real, imag = jnp.zeros((8, 256), F32), jnp.zeros((8, 256), F32)
    for c in range(N):
        ur, ui = u[8 * c:8 * c + 8, :256], u[8 * c:8 * c + 8, 256:]
        tc, ts = tw_c[c:c + 1, :], tw_s[c:c + 1, :]
        real += ur * tc + ui * ts
        imag += ui * tc - ur * ts
    return real, imag


def x_table(bx0, bx1, tc, ts):
    return split(bx0 * tc + bx1 * ts)


def forward_x(real, imag, bx_hi, bx_lo, roll):
    low = lax.broadcasted_iota(jnp.int32, (8, 128), 1) < 64
    rows = []
    for v in range(2):
        re, im = real[:, 128 * v:128 * v + 128], imag[:, 128 * v:128 * v + 128]
        rows.append(jnp.where(low, re, roll(im, 64, 1)))
        rows.append(jnp.where(low, roll(re, 64, 1), im))
    hi, lo = split(jnp.concatenate(rows, 0))
    u = dot(jnp.concatenate([hi, lo], 0), bx_hi)
    return u[:32] + u[32:] + dot(hi, bx_lo)


def lifted_coeffs(total, first, lift):
    row = lax.broadcasted_iota(jnp.int32, (8, 128), 0)
    lane = lax.broadcasted_iota(jnp.int32, (8, 128), 1)
    total = total * (1.0 / 8388608.0) + jnp.where((row == 3) & (lane == 0), first, 0.0)
    return lax.dot_general(
        total.T, lift, (((1,), (1,)), ((), ())), precision=lax.Precision.HIGHEST,
        preferred_element_type=F32,
    )


def mix(coeffs, weight, sel):
    his, los = [], []
    for ky in range(2):
        for kz in range(2):
            cr = coeffs[64 * ky:64 * ky + 32, 128 * kz:128 * kz + 128]
            ci = coeffs[64 * ky + 32:64 * ky + 64, 128 * kz:128 * kz + 128]
            cr8 = jnp.concatenate([cr] * 8, 1)
            ci8 = jnp.concatenate([ci] * 8, 1)
            wr = weight(0, ky, kz).astype(F32)
            wi = weight(1, ky, kz).astype(F32)
            for value in (wr * cr8 - wi * ci8, wr * ci8 + wi * cr8):
                hi, lo = split(value)
                his.append(hi)
                los.append(lo)
    return dot(jnp.concatenate(his, 0), sel) + dot(jnp.concatenate(los, 0), sel)


def inverse_x(mixed, ky, inv_x):
    kind = lax.broadcasted_iota(jnp.int32, (32, 128), 1) % 4
    block = [mixed[128 * ky + 32 * n:128 * ky + 32 * n + 32] for n in range(4)]

    def pick(a, b, c, d):
        return jnp.where(kind == 0, a, jnp.where(kind == 1, b, jnp.where(kind == 2, c, d)))

    top = pick(block[0], block[1], block[2], block[3])
    bottom = pick(-block[1], block[0], -block[3], block[2])
    hi, lo = split(jnp.concatenate([top, bottom], 0))
    return dot(inv_x, jnp.concatenate([hi, lo, hi], 0))


def turned(arrived, roll):
    even = lax.broadcasted_iota(jnp.int32, arrived.shape, 1) % 2 == 0
    other = jnp.where(even, roll(arrived, 127, 1), -roll(arrived, 1, 1))
    return arrived.T, other.T


def inverse_y(plain, other, tc, ts, ey_hi, ey_lo):
    hi, lo = split(jnp.concatenate([plain * tc - other * ts, other * tc + plain * ts], 1))
    return dot(hi, ey_hi) + dot(lo, ey_hi) + dot(hi, ey_lo)


def inverse_z(block, inv_z):
    hi, lo = split(block.T)
    return dot(jnp.concatenate([hi, lo, hi], 1), inv_z)


def activate(value):
    cubic = value * (0.7978845608028654 + 0.035677408136300125 * (value * value))
    half = 0.5 * value
    return half + half * jnp.tanh(cubic)


def exchange_kernel(
    step_ref, v_hbm, t_hbm, w_hbm, lift_ref, fz_hbm, by_hbm, twy_hbm, bx_hbm, twx_hbm, sel_hbm,
    ix_hbm, ey_hbm, twi_hbm,
    out_ref,
    v_ref, t_ref, w_ref, fz_ref, by_ref, twy_ref, bx_ref, twx_ref, sel_ref, ix_ref, ey_ref, twi_ref,
    s1, r1, s2, r2, s3, r3, s4,
    load_sem, send1, recv1, send2, recv2, send3, recv3, send4, recv4,
):
    r = lax.axis_index("row")
    c = lax.axis_index("col")

    barrier = pltpu.get_barrier_semaphore()
    pairs = [
        (v_hbm, v_ref), (t_hbm, t_ref), (fz_hbm, fz_ref), (by_hbm, by_ref), (twy_hbm, twy_ref),
        (bx_hbm, bx_ref), (twx_hbm, twx_ref), (w_hbm, w_ref), (sel_hbm, sel_ref), (ix_hbm, ix_ref),
        (ey_hbm, ey_ref), (twi_hbm, twi_ref),
    ]
    loads = [
        pltpu.make_async_copy(src, dst, load_sem.at[n]) for n, (src, dst) in enumerate(pairs)
    ]
    for load in loads:
        load.start()
    for d in range(1, N):
        pl.semaphore_signal(
            barrier, inc=1, device_id={"row": r, "col": (c + d) % N}, device_id_type=MESH)
        pl.semaphore_signal(
            barrier, inc=1, device_id={"row": (r + d) % N, "col": c}, device_id_type=MESH)

    for load in loads[:3]:
        load.wait()
    advanced = (v_ref[...] + step_ref[0] * t_ref[...]).reshape(384, 256)
    z = forward_z(advanced, fz_ref[...])
    s1[pl.ds(3, 64, stride=4), :] = jnp.zeros((64, 128), F32)
    for j in range(3):
        s1[pl.ds(j, 64, stride=4), :] = z[:, 128 * j:128 * j + 128]
    pl.semaphore_wait(barrier, 2 * (N - 1))

    def to_col(src, dst, send, recv, d):
        return pltpu.make_async_remote_copy(
            src_ref=src, dst_ref=dst, send_sem=send, recv_sem=recv,
            device_id={"row": r, "col": d}, device_id_type=MESH)

    def to_row(src, dst, send, recv, d):
        return pltpu.make_async_remote_copy(
            src_ref=src, dst_ref=dst, send_sem=send, recv_sem=recv,
            device_id={"row": d, "col": c}, device_id_type=MESH)

    first = []
    for d in range(1, N):
        dest = (c + d) % N
        for part in range(2):
            first.append(to_col(
                s1.at[pl.ds(pl.multiple_of(128 * part + 8 * dest, 8), 8)], r1.at[part, c],
                send1.at[part, d], recv1.at[part, d], dest))
            first[-1].start()
    for part in range(2):
        r1[part, c] = s1[pl.ds(pl.multiple_of(128 * part + 8 * c, 8), 8), :]
    for load in loads[3:]:
        load.wait()
    bx_hi, bx_lo = x_table(
        bx_ref[0], bx_ref[1], twx_ref[0, pl.ds(r, 1), :], twx_ref[1, pl.ds(r, 1), :])
    for copy in first:
        copy.wait_recv()

    arrived = jnp.concatenate([r1[0].reshape(128, 128), r1[1].reshape(128, 128)], 1)
    real, imag = forward_y(arrived, by_ref[0], by_ref[1], twy_ref[0], twy_ref[1])
    partial = forward_x(real, imag, bx_hi, bx_lo, pltpu.roll)
    for g in range(4):
        for k in range(4):
            s2[4 * g + k] = partial[8 * g:8 * g + 8, 128 * k:128 * k + 128]
    second = []
    for d in range(1, N):
        dest = (r + d) % N
        second.append(to_row(s2.at[dest], r2.at[r], send2.at[d], recv2.at[d], dest))
        second[-1].start()
    r2[r] = s2[r]
    for copy in second:
        copy.wait_recv()
    total = jnp.sum(r2[...], axis=0)

    origin = jnp.where((r == 0) & (c == 0), 1.0, 0.0).astype(F32)
    coeffs = lifted_coeffs(total, origin, lift_ref[...])
    mixed = mix(coeffs, lambda part, ky, kz: w_ref[part, ky, kz], sel_ref[...])
    for ky in range(2):
        s3[:, 8 * ky:8 * ky + 8, :] = inverse_x(mixed, ky, ix_ref[...]).reshape(16, 8, 128)
    third = []
    for d in range(1, N):
        dest = (r + d) % N
        third.append(to_row(s3.at[dest], r3.at[r], send3.at[d], recv3.at[d], dest))
        third[-1].start()
    r3[r] = s3[r]
    for copy in third:
        copy.wait_recv()

    plain, other = turned(r3[...].reshape(256, 128), pltpu.roll)
    for k in range(8):
        m = (c // 2 + k) % 8
        h = inverse_y(plain, other, twi_ref[0, pl.ds(m, 1), :], twi_ref[1, pl.ds(m, 1), :],
                      ey_ref[0], ey_ref[1])
        for b in range(2):
            dest = 2 * m + b
            s4[dest] = h[:, 128 * b:128 * b + 128]
            copy = to_col(s4.at[dest], out_ref.at[c], send4.at[dest], recv4.at[c], dest)
            if k > 0:
                copy.start()
            else:
                @pl.when(dest != c)
                def _():
                    copy.start()

    out_ref[c] = s4[c]
    for d in range(1, N):
        source = (c + d) % N
        copy = to_col(s4.at[source], out_ref.at[source], send4.at[source], recv4.at[source], source)
        copy.wait_recv()
        copy.wait_send()
    for copy in first + second + third:
        copy.wait_send()


def cells_kernel(step_ref, local_ref, g_ref, v_ref, t_ref, iz_ref, out_ref, adv_ref):
    @pl.when(pl.program_id(0) == 0)
    def _():
        adv_ref[...] = v_ref[...] + step_ref[0] * t_ref[...]

    base = pl.program_id(0) * 8
    for q in range(4):
        values = inverse_z(g_ref[:, 8 * q:8 * q + 8, :].reshape(128, 128), iz_ref[...])
        for o in range(2):
            index = base + 2 * q + o
            scale = [local_ref[index, j] for j in range(4)]
            for x in range(8):
                cell = slice(16 * x, 16 * x + 16)
                value = values[cell, 256 * o:256 * o + 256] + scale[3]
                for j in range(3):
                    value += scale[j] * adv_ref[j, cell, :]
                out_ref[2 * q + o, x] = activate(value).astype(BF16)


def per_device(
    velocity, tendency, step_size, lift_weight, lift_bias, spectral_weight, local_weight, local_bias
):
    highest = lax.Precision.HIGHEST
    t = tables()
    v = velocity.reshape(3, 128, 256)
    dv = tendency.reshape(3, 128, 256)
    four = jnp.concatenate([lift_weight, lift_bias[:, None]], 1)
    four = jnp.concatenate([four] * 4, 0)
    zero = jnp.zeros((128, 4), F32)
    lift = jnp.concatenate(
        [jnp.concatenate([four, zero], 1), jnp.concatenate([zero, four], 1)], 0)
    local = jnp.dot(local_weight, four[:32], precision=highest)
    local = local + jnp.concatenate([jnp.zeros((32, 3), F32), local_bias[:, None]], 1)

    vmem = pl.BlockSpec(memory_space=pltpu.VMEM)
    smem = pl.BlockSpec(memory_space=pltpu.SMEM)
    anywhere = pl.BlockSpec(memory_space=pl.ANY)
    far = [v, dv, spectral_weight]
    consts = [t[n] for n in ("fwd_z", "by", "tw_y", "bx", "tw_x", "sel", "inv_x", "ey", "tw_i")]
    scratch = [pltpu.VMEM(a.shape, a.dtype) for a in far + consts]
    blocks = pl.pallas_call(
        exchange_kernel,
        out_shape=jax.ShapeDtypeStruct((16, 128, 128), F32),
        in_specs=[smem] + [anywhere] * 3 + [vmem] + [anywhere] * len(consts),
        out_specs=vmem,
        scratch_shapes=scratch + [
            pltpu.VMEM((256, 128), F32), pltpu.VMEM((2, 16, 8, 128), F32),
            pltpu.VMEM((16, 8, 128), F32), pltpu.VMEM((16, 8, 128), F32),
            pltpu.VMEM((16, 16, 128), F32), pltpu.VMEM((16, 16, 128), F32),
            pltpu.VMEM((16, 128, 128), F32),
            pltpu.SemaphoreType.DMA((12,)),
            pltpu.SemaphoreType.DMA((2, 16)), pltpu.SemaphoreType.DMA((2, 16)),
        ] + [pltpu.SemaphoreType.DMA((16,))] * 6,
        compiler_params=pltpu.CompilerParams(
            collective_id=0, has_side_effects=True, vmem_limit_bytes=40 * 1024 * 1024),
        name="exchange",
    )(step_size, *far, lift, *[jnp.asarray(a) for a in consts])

    out = pl.pallas_call(
        cells_kernel,
        grid=(4,),
        out_shape=jax.ShapeDtypeStruct((32, 8, 16, 256), BF16),
        in_specs=[
            smem, smem,
            pl.BlockSpec((16, 32, 128), lambda i: (0, i, 0)),
            pl.BlockSpec((3, 128, 256), lambda i: (0, 0, 0)),
            pl.BlockSpec((3, 128, 256), lambda i: (0, 0, 0)),
            pl.BlockSpec((384, 512), lambda i: (0, 0)),
        ],
        out_specs=pl.BlockSpec((8, 8, 16, 256), lambda i: (i, 0, 0, 0)),
        scratch_shapes=[pltpu.VMEM((3, 128, 256), F32)],
        compiler_params=pltpu.CompilerParams(vmem_limit_bytes=40 * 1024 * 1024),
        name="cells",
    )(step_size, local, blocks, v, dv, jnp.asarray(t["inv_z"]))
    return out.reshape(1, 32, 8, 16, 256)


def solution(mesh):
    in_specs = (
        P(None, None, "row", "col", None),
        P(None, None, "row", "col", None),
        P(),
        P(),
        P(),
        P(None, "row", "col", None, None),
        P(),
        P(),
    )
    out_specs = P(None, None, "row", "col", None)
    return jax.shard_map(
        per_device, mesh=mesh, in_specs=in_specs, out_specs=out_specs, check_vma=False
    )
```

```python
import functools
import math

import jax
import jax.numpy as jnp
import numpy as np
from jax import lax
from jax.experimental import pallas as pl
from jax.experimental.pallas import tpu as pltpu
from jax.sharding import PartitionSpec as P

F32 = jnp.float32
BF16 = jnp.bfloat16
MESH = pl.DeviceIdType.MESH
VMEM_LIMIT = 60 * 1024 * 1024
N = 16


def split(x):
    hi = x.astype(BF16)
    lo = (x - hi.astype(F32)).astype(BF16)
    return hi, lo


def dot(a, b):
    return jnp.dot(a, b, preferred_element_type=F32)


def dot_nt(a, b):
    return lax.dot_general(a, b, (((1,), (1,)), ((), ())), preferred_element_type=F32)


def dot_exact(a, b):
    return jnp.dot(a, b, precision=lax.Precision.HIGHEST, preferred_element_type=F32)


def np_split(x):
    x = np.asarray(x, np.float64)
    hi = x.astype(np.float32).astype(jnp.bfloat16)
    lo = (x - hi.astype(np.float64)).astype(np.float32).astype(jnp.bfloat16)
    return hi, lo


@functools.lru_cache(None)
def tables():
    turn = 2.0 * np.pi
    ix = np.arange
    waves = np.where(ix(32) < 16, ix(32), ix(32) - 32)
    eye8 = np.eye(8)
    z_angle = turn * (ix(32)[:, None] * ix(256)[None, :] % 256) / 256
    z_hi, z_lo = np_split(np.concatenate([np.cos(z_angle), -np.sin(z_angle)], 0))
    fwd_z = np.concatenate([z_hi, z_lo, z_hi], 1)
    a = turn * waves[None, :] * ix(16)[:, None] / 256
    by = np.zeros((2, 8, 16, 2, 32, 8))
    for x in range(8):
        by[0, x, :, 0, :, x] = np.cos(a)
        by[1, x, :, 0, :, x] = np.sin(a)
        by[0, x, :, 1, :, x] = -np.sin(a)
        by[1, x, :, 1, :, x] = np.cos(a)
    by_hi, by_lo = np_split(by.reshape(256, 512))
    b = turn * (waves[None, :] * ix(16)[:, None] % 16) / 16
    b = np.repeat(b, 8, axis=1)
    tw_y = np.stack([np.cos(b), np.sin(b)], 0).astype(np.float32)
    c = turn * waves[None, :] * ix(8)[:, None] / 128
    bx = []
    for quarter in (0.0, np.pi / 2):
        t = np.zeros((2, 8, 8, 8, 2, 32))
        for e in range(8):
            t[0, e, :, e, 0, :] = np.cos(c + quarter)
            t[1, e, :, e, 0, :] = np.sin(c + quarter)
            t[0, e, :, e, 1, :] = -np.sin(c + quarter)
            t[1, e, :, e, 1, :] = np.cos(c + quarter)
        bx.append(t.reshape(128, 512))
    bx = np.stack(bx, 0).astype(np.float32)
    d = turn * (waves[None, :] * ix(16)[:, None] % 16) / 16
    d = np.tile(d, (1, 16))
    tw_x = np.stack([np.cos(d), np.sin(d)], 0).astype(np.float32)
    sel = (ix(1024)[:, None] // 32 == ix(128)[None, :] // 4).astype(jnp.bfloat16)
    f = turn * (waves[None, :] * ix(128)[:, None] % 128) / 128
    ex_hi, ex_lo = np_split(np.concatenate([np.cos(f), np.sin(f)], 1))
    inv_x = np.concatenate([ex_hi, ex_hi, ex_lo], 1)
    g = turn * waves[:, None] * ix(32)[None, :] / 256
    ey = np.zeros((2, 32, 8, 2, 8, 16))
    for x in range(8):
        for blk in range(2):
            ey[0, :, x, blk, x, :] = np.cos(g[:, blk * 16:blk * 16 + 16])
            ey[1, :, x, blk, x, :] = -np.sin(g[:, blk * 16:blk * 16 + 16])
    ey_hi, ey_lo = np_split(ey.reshape(512, 256))
    h = turn * (waves[None, :] * ix(8)[:, None] % 8) / 8
    h = np.repeat(h, 8, axis=1)
    tw_i = np.stack([np.cos(h), np.sin(h)], 0).astype(np.float32)
    ez = np.zeros((16, 2, 2, 2, 2, 256))
    weight = np.where(ix(32) == 0, 1.0, 2.0)[:, None]
    cz = (weight * np.cos(z_angle)).reshape(16, 2, 256)
    sz = (-weight * np.sin(z_angle)).reshape(16, 2, 256)
    for o in range(2):
        ez[:, o, :, 0, o, :] = cz
        ez[:, o, :, 1, o, :] = sz
    ez_hi, ez_lo = np_split(ez.reshape(128, 512))
    inv_z = np.concatenate([ez_hi, ez_hi, ez_lo], 0)
    return dict(
        fwd_z=fwd_z, by=np.stack([by_hi, by_lo], 0), tw_y=tw_y, bx=bx, tw_x=tw_x, sel=sel,
        inv_x=inv_x, ey=np.stack([ey_hi, ey_lo], 0), tw_i=tw_i, inv_z=inv_z,
    )


def forward_z(advanced, fwd_z):
    hi, lo = split(advanced)
    return dot_nt(fwd_z, jnp.concatenate([hi, hi, lo], 1))


def forward_y(arrived, by_hi, by_lo, tw_c, tw_s):
    hi, lo = split(arrived)
    u = dot(jnp.concatenate([hi, lo], 0), by_hi)
    u = u[:128] + u[128:] + dot(hi, by_lo)
    real, imag = jnp.zeros((8, 256), F32), jnp.zeros((8, 256), F32)
    for c in range(N):
        ur, ui = u[8 * c:8 * c + 8, :256], u[8 * c:8 * c + 8, 256:]
        tc, ts = tw_c[c:c + 1, :], tw_s[c:c + 1, :]
        real += ur * tc + ui * ts
        imag += ui * tc - ur * ts
    return real, imag


def x_table(bx0, bx1, tc, ts):
    return split(bx0 * tc + bx1 * ts)


def forward_x(real, imag, bx_hi, bx_lo, roll):
    low = lax.broadcasted_iota(jnp.int32, (8, 128), 1) < 64
    rows = []
    for v in range(2):
        re, im = real[:, 128 * v:128 * v + 128], imag[:, 128 * v:128 * v + 128]
        rows.append(jnp.where(low, re, roll(im, 64, 1)))
        rows.append(jnp.where(low, roll(re, 64, 1), im))
    hi, lo = split(jnp.concatenate(rows, 0))
    u = dot(jnp.concatenate([hi, lo], 0), bx_hi)
    return u[:32] + u[32:] + dot(hi, bx_lo)


def lift_table(rows):
    i = lax.broadcasted_iota(jnp.int32, (32, 128), 0)
    lane = lax.broadcasted_iota(jnp.int32, (32, 128), 1)
    wide = dot_exact(rows, jnp.where(lane % 32 == i, 1.0, 0.0).astype(F32))
    upper = lax.broadcasted_iota(jnp.int32, (8, 128), 0) < 4
    return jnp.concatenate([jnp.where(upper, wide, 0.0), jnp.where(upper, 0.0, wide)], 1)


def local_table(rows, local_weight, local_bias):
    wide = jnp.concatenate([jnp.broadcast_to(rows[j:j + 1], (128, 32)) for j in range(4)], 0)
    scale = lax.dot_general(
        local_weight, wide, (((1,), (1,)), ((), ())), precision=lax.Precision.HIGHEST,
        preferred_element_type=F32)
    same = lax.broadcasted_iota(jnp.int32, (32, 32), 0) == lax.broadcasted_iota(
        jnp.int32, (32, 32), 1)
    bias = lax.dot_general(
        jnp.where(same, 1.0, 0.0).astype(F32), jnp.broadcast_to(local_bias, (128, 32)),
        (((1,), (1,)), ((), ())), precision=lax.Precision.HIGHEST, preferred_element_type=F32)
    return jnp.concatenate([scale[:, :384], scale[:, 384:] + bias], 1)


def lifted_coeffs(total, first, lift):
    row = lax.broadcasted_iota(jnp.int32, (8, 128), 0)
    lane = lax.broadcasted_iota(jnp.int32, (8, 128), 1)
    total = total * (1.0 / 8388608.0) + jnp.where((row == 3) & (lane == 0), first, 0.0)
    return dot_exact(total.T, lift)


def mix(coeffs, weight, sel):
    his, los = [], []
    for ky in range(2):
        for kz in range(2):
            cr = coeffs[64 * ky:64 * ky + 32, 128 * kz:128 * kz + 128]
            ci = coeffs[64 * ky + 32:64 * ky + 64, 128 * kz:128 * kz + 128]
            cr8 = jnp.concatenate([cr] * 8, 1)
            ci8 = jnp.concatenate([ci] * 8, 1)
            wr = weight(0, ky, kz).astype(F32)
            wi = weight(1, ky, kz).astype(F32)
            for value in (wr * cr8 - wi * ci8, wr * ci8 + wi * cr8):
                hi, lo = split(value)
                his.append(hi)
                los.append(lo)
    return dot(jnp.concatenate(his, 0), sel) + dot(jnp.concatenate(los, 0), sel)


def inverse_x(mixed, ky, inv_x):
    kind = lax.broadcasted_iota(jnp.int32, (32, 128), 1) % 4
    block = [mixed[128 * ky + 32 * n:128 * ky + 32 * n + 32] for n in range(4)]

    def pick(a, b, c, d):
        return jnp.where(kind == 0, a, jnp.where(kind == 1, b, jnp.where(kind == 2, c, d)))

    top = pick(block[0], block[1], block[2], block[3])
    bottom = pick(-block[1], block[0], -block[3], block[2])
    hi, lo = split(jnp.concatenate([top, bottom], 0))
    return dot(inv_x, jnp.concatenate([hi, lo, hi], 0))


def turned(arrived, roll):
    even = lax.broadcasted_iota(jnp.int32, arrived.shape, 1) % 2 == 0
    other = jnp.where(even, roll(arrived, 127, 1), -roll(arrived, 1, 1))
    return arrived.T, other.T


def inverse_y(plain, other, tc, ts, ey_hi, ey_lo):
    hi, lo = split(jnp.concatenate([plain * tc - other * ts, other * tc + plain * ts], 1))
    return dot(hi, ey_hi) + dot(lo, ey_hi) + dot(hi, ey_lo)


def inverse_z(block, inv_z):
    hi, lo = split(block.T)
    return dot(jnp.concatenate([hi, lo, hi], 1), inv_z)


def activate(value):
    cubic = value * (0.7978845608028654 + 0.035677408136300125 * (value * value))
    half = 0.5 * value
    return half + half * jnp.tanh(cubic)


def exchange_kernel(
    *refs,
):
    hbm, refs = refs[:17], refs[17:]
    (out_ref, local_ref, adv_ref), refs = refs[:3], refs[3:]
    local, refs = refs[:17], refs[17:]
    (step_ref, v_ref, t_ref, fz_ref, by_ref, twy_ref, bx_ref, twx_ref, lift_ref, bias_ref, w_ref,
     sel_ref, ix_ref, ey_ref, twi_ref, lw_ref, lb_ref) = local
    (s1, r1, s2, r2, s3, r3, s4, rows_ref,
     load_sem, send1, recv1, send2, recv2, send3, recv3, send4, recv4) = refs
    r = lax.axis_index("row")
    c = lax.axis_index("col")

    barrier = pltpu.get_barrier_semaphore()
    loads = [
        pltpu.make_async_copy(src, dst, load_sem.at[n]) for n, (src, dst) in enumerate(zip(hbm, local))
    ]
    for load in loads:
        load.start()
    for d in range(1, N):
        pl.semaphore_signal(
            barrier, inc=1, device_id={"row": r, "col": (c + d) % N}, device_id_type=MESH)
        pl.semaphore_signal(
            barrier, inc=1, device_id={"row": (r + d) % N, "col": c}, device_id_type=MESH)

    for load in loads[:4]:
        load.wait()
    advanced = v_ref[...] + step_ref[0] * t_ref[...]
    adv_ref[...] = advanced
    advanced = advanced.reshape(384, 256)
    z = forward_z(advanced, fz_ref[...])
    s1[pl.ds(3, 64, stride=4), :] = jnp.zeros((64, 128), F32)
    for j in range(3):
        s1[pl.ds(j, 64, stride=4), :] = z[:, 128 * j:128 * j + 128]
    pl.semaphore_wait(barrier, 2 * (N - 1))

    def to_col(src, dst, send, recv, d):
        return pltpu.make_async_remote_copy(
            src_ref=src, dst_ref=dst, send_sem=send, recv_sem=recv,
            device_id={"row": r, "col": d}, device_id_type=MESH)

    def to_row(src, dst, send, recv, d):
        return pltpu.make_async_remote_copy(
            src_ref=src, dst_ref=dst, send_sem=send, recv_sem=recv,
            device_id={"row": d, "col": c}, device_id_type=MESH)

    first = []
    for d in range(1, N):
        dest = (c + d) % N
        for part in range(2):
            first.append(to_col(
                s1.at[pl.ds(pl.multiple_of(128 * part + 8 * dest, 8), 8)], r1.at[part, c],
                send1.at[part, d], recv1.at[part, d], dest))
            first[-1].start()
    for part in range(2):
        r1[part, c] = s1[pl.ds(pl.multiple_of(128 * part + 8 * c, 8), 8), :]
    for load in loads[4:]:
        load.wait()
    bx_hi, bx_lo = x_table(
        bx_ref[0], bx_ref[1], twx_ref[0, pl.ds(r, 1), :], twx_ref[1, pl.ds(r, 1), :])
    for k in (0, 4):
        rows_ref[k:k + 3] = lift_ref[...]
        rows_ref[k + 3:k + 4] = bias_ref[...]
    lift = lift_table(rows_ref[...])
    local_ref[...] = local_table(rows_ref[...], lw_ref[...], lb_ref[...])
    for copy in first:
        copy.wait_recv()

    arrived = jnp.concatenate([r1[0].reshape(128, 128), r1[1].reshape(128, 128)], 1)
    real, imag = forward_y(arrived, by_ref[0], by_ref[1], twy_ref[0], twy_ref[1])
    partial = forward_x(real, imag, bx_hi, bx_lo, pltpu.roll)
    for g in range(4):
        for k in range(4):
            s2[4 * g + k] = partial[8 * g:8 * g + 8, 128 * k:128 * k + 128]
    second = []
    for d in range(1, N):
        dest = (r + d) % N
        second.append(to_row(s2.at[dest], r2.at[r], send2.at[d], recv2.at[d], dest))
        second[-1].start()
    r2[r] = s2[r]
    for copy in second:
        copy.wait_recv()
    total = jnp.sum(r2[...], axis=0)

    origin = jnp.where((r == 0) & (c == 0), 1.0, 0.0).astype(F32)
    coeffs = lifted_coeffs(total, origin, lift)
    mixed = mix(coeffs, lambda part, ky, kz: w_ref[part, ky, kz], sel_ref[...])
    for ky in range(2):
        s3[:, 8 * ky:8 * ky + 8, :] = inverse_x(mixed, ky, ix_ref[...]).reshape(16, 8, 128)
    third = []
    for d in range(1, N):
        dest = (r + d) % N
        third.append(to_row(s3.at[dest], r3.at[r], send3.at[d], recv3.at[d], dest))
        third[-1].start()
    r3[r] = s3[r]
    for copy in third:
        copy.wait_recv()

    plain, other = turned(r3[...].reshape(256, 128), pltpu.roll)
    for k in range(8):
        m = (c // 2 + k) % 8
        h = inverse_y(plain, other, twi_ref[0, pl.ds(m, 1), :], twi_ref[1, pl.ds(m, 1), :],
                      ey_ref[0], ey_ref[1])
        for b in range(2):
            dest = 2 * m + b
            s4[dest] = h[:, 128 * b:128 * b + 128]
            copy = to_col(s4.at[dest], out_ref.at[c], send4.at[dest], recv4.at[c], dest)
            if k > 0:
                copy.start()
            else:
                @pl.when(dest != c)
                def _():
                    copy.start()

    out_ref[c] = s4[c]
    for d in range(1, N):
        source = (c + d) % N
        copy = to_col(s4.at[source], out_ref.at[source], send4.at[source], recv4.at[source], source)
        copy.wait_recv()
        copy.wait_send()
    for copy in first + second + third:
        copy.wait_send()


def cells_kernel(local_ref, g_ref, adv_ref, iz_ref, out_ref):
    for q in range(4):
        values = inverse_z(g_ref[:, 8 * q:8 * q + 8, :].reshape(128, 128), iz_ref[...])
        for o in range(2):
            index = 2 * q + o
            scale = [
                jnp.concatenate([local_ref[index:index + 1, 128 * j:128 * j + 128]] * 2, 1)
                for j in range(4)
            ]
            for x in range(8):
                cell = slice(16 * x, 16 * x + 16)
                value = values[cell, 256 * o:256 * o + 256] + scale[3]
                for j in range(3):
                    value += scale[j] * adv_ref[j, cell, :]
                out_ref[2 * q + o, x] = activate(value).astype(BF16)


def per_device(
    velocity, tendency, step_size, lift_weight, lift_bias, spectral_weight, local_weight, local_bias
):
    t = tables()
    v = velocity.reshape(3, 128, 256)
    dv = tendency.reshape(3, 128, 256)
    vmem = pl.BlockSpec(memory_space=pltpu.VMEM)
    anywhere = pl.BlockSpec(memory_space=pl.ANY)
    const = {name: jnp.asarray(a) for name, a in t.items()}
    far = [
        step_size, v, dv, const["fwd_z"], const["by"], const["tw_y"], const["bx"], const["tw_x"],
        lift_weight.T, lift_bias[None, :], spectral_weight, const["sel"], const["inv_x"],
        const["ey"], const["tw_i"], local_weight, local_bias[None, :],
    ]
    scratch = [pltpu.SMEM((1,), F32)] + [pltpu.VMEM(a.shape, a.dtype) for a in far[1:]]
    blocks, local, advanced = pl.pallas_call(
        exchange_kernel,
        out_shape=(
            jax.ShapeDtypeStruct((16, 128, 128), F32), jax.ShapeDtypeStruct((32, 512), F32),
            jax.ShapeDtypeStruct((3, 128, 256), F32)),
        in_specs=[anywhere] * len(far),
        out_specs=(vmem, vmem, vmem),
        scratch_shapes=scratch + [
            pltpu.VMEM((256, 128), F32), pltpu.VMEM((2, 16, 8, 128), F32),
            pltpu.VMEM((16, 8, 128), F32), pltpu.VMEM((16, 8, 128), F32),
            pltpu.VMEM((16, 16, 128), F32), pltpu.VMEM((16, 16, 128), F32),
            pltpu.VMEM((16, 128, 128), F32), pltpu.VMEM((8, 32), F32),
            pltpu.SemaphoreType.DMA((len(far),)),
            pltpu.SemaphoreType.DMA((2, 16)), pltpu.SemaphoreType.DMA((2, 16)),
        ] + [pltpu.SemaphoreType.DMA((16,))] * 6,
        compiler_params=pltpu.CompilerParams(
            collective_id=0, has_side_effects=True, vmem_limit_bytes=VMEM_LIMIT),
        name="exchange",
    )(*far)

    out = pl.pallas_call(
        cells_kernel,
        grid=(4,),
        out_shape=jax.ShapeDtypeStruct((32, 8, 16, 256), BF16),
        in_specs=[
            pl.BlockSpec((8, 512), lambda i: (i, 0)),
            pl.BlockSpec((16, 32, 128), lambda i: (0, i, 0)),
            pl.BlockSpec((3, 128, 256), lambda i: (0, 0, 0)),
            pl.BlockSpec((384, 512), lambda i: (0, 0)),
        ],
        out_specs=pl.BlockSpec((8, 8, 16, 256), lambda i: (i, 0, 0, 0)),
        compiler_params=pltpu.CompilerParams(vmem_limit_bytes=VMEM_LIMIT),
        name="cells",
    )(local, blocks, advanced, const["inv_z"])
    return out.reshape(1, 32, 8, 16, 256)


def solution(mesh):
    in_specs = (
        P(None, None, "row", "col", None),
        P(None, None, "row", "col", None),
        P(),
        P(),
        P(),
        P(None, "row", "col", None, None),
        P(),
        P(),
    )
    out_specs = P(None, None, "row", "col", None)
    return jax.shard_map(
        per_device, mesh=mesh, in_specs=in_specs, out_specs=out_specs, check_vma=False
    )
```

```python
import functools
import math

import jax
import jax.numpy as jnp
import numpy as np
from jax import lax
from jax.experimental import pallas as pl
from jax.experimental.pallas import tpu as pltpu
from jax.sharding import PartitionSpec as P

F32 = jnp.float32
BF16 = jnp.bfloat16
MESH = pl.DeviceIdType.MESH
VMEM_LIMIT = 60 * 1024 * 1024
N = 16


def split(x):
    hi = x.astype(BF16)
    lo = (x - hi.astype(F32)).astype(BF16)
    return hi, lo


def dot(a, b):
    return jnp.dot(a, b, preferred_element_type=F32)


def dot_nt(a, b):
    return lax.dot_general(a, b, (((1,), (1,)), ((), ())), preferred_element_type=F32)


def dot_exact(a, b):
    return jnp.dot(a, b, precision=lax.Precision.HIGHEST, preferred_element_type=F32)


def np_split(x):
    x = np.asarray(x, np.float64)
    hi = x.astype(np.float32).astype(jnp.bfloat16)
    lo = (x - hi.astype(np.float64)).astype(np.float32).astype(jnp.bfloat16)
    return hi, lo


@functools.lru_cache(None)
def tables():
    turn = 2.0 * np.pi
    ix = np.arange
    waves = np.where(ix(32) < 16, ix(32), ix(32) - 32)
    eye8 = np.eye(8)
    z_angle = turn * (ix(32)[:, None] * ix(256)[None, :] % 256) / 256
    z_hi, z_lo = np_split(np.concatenate([np.cos(z_angle), -np.sin(z_angle)], 0))
    fwd_z = np.concatenate([z_hi, z_lo, z_hi], 1)
    fwd_z = fwd_z.reshape(2, 16, 2, 768).transpose(1, 0, 2, 3).reshape(64, 768)
    a = turn * waves[None, :] * ix(16)[:, None] / 256
    by = np.zeros((2, 8, 16, 2, 32, 8))
    for x in range(8):
        by[0, x, :, 0, :, x] = np.cos(a)
        by[1, x, :, 0, :, x] = np.sin(a)
        by[0, x, :, 1, :, x] = -np.sin(a)
        by[1, x, :, 1, :, x] = np.cos(a)
    by_hi, by_lo = np_split(by.reshape(256, 512))
    b = turn * (waves[None, :] * ix(16)[:, None] % 16) / 16
    b = np.repeat(b, 8, axis=1)
    tw_y = np.stack([np.cos(b), np.sin(b)], 0).astype(np.float32)
    c = turn * waves[None, :] * ix(8)[:, None] / 128
    bx = []
    for quarter in (0.0, np.pi / 2):
        t = np.zeros((2, 8, 8, 8, 2, 32))
        for e in range(8):
            t[0, e, :, e, 0, :] = np.cos(c + quarter)
            t[1, e, :, e, 0, :] = np.sin(c + quarter)
            t[0, e, :, e, 1, :] = -np.sin(c + quarter)
            t[1, e, :, e, 1, :] = np.cos(c + quarter)
        bx.append(t.reshape(128, 512))
    bx = np.stack(bx, 0).astype(np.float32)
    d = turn * (waves[None, :] * ix(16)[:, None] % 16) / 16
    d = np.tile(d, (1, 16))
    tw_x = np.stack([np.cos(d), np.sin(d)], 0).astype(np.float32)
    sel = (ix(512)[:, None] // 32 == ix(128)[None, :] // 4 % 16).astype(jnp.bfloat16)
    f = turn * (waves[None, :] * ix(128)[:, None] % 128) / 128
    ex_hi, ex_lo = np_split(np.concatenate([np.cos(f), np.sin(f)], 1))
    inv_x = np.concatenate([ex_hi, ex_hi, ex_lo], 1)
    g = turn * waves[:, None] * ix(32)[None, :] / 256
    ey = np.zeros((2, 32, 8, 2, 8, 16))
    for x in range(8):
        for blk in range(2):
            ey[0, :, x, blk, x, :] = np.cos(g[:, blk * 16:blk * 16 + 16])
            ey[1, :, x, blk, x, :] = -np.sin(g[:, blk * 16:blk * 16 + 16])
    ey = ey.reshape(2, 16, 2, 8, 256).transpose(0, 2, 1, 3, 4)
    ey_hi, ey_lo = np_split(ey.reshape(512, 256))
    h = turn * (waves[None, :] * ix(8)[:, None] % 8) / 8
    h = np.repeat(h.reshape(8, 16, 2).transpose(0, 2, 1).reshape(8, 32), 8, axis=1)
    tw_i = np.stack([np.cos(h), np.sin(h)], 0).astype(np.float32)
    ez = np.zeros((16, 2, 2, 2, 2, 256))
    weight = np.where(ix(32) == 0, 1.0, 2.0)[:, None]
    cz = (weight * np.cos(z_angle)).reshape(16, 2, 256)
    sz = (-weight * np.sin(z_angle)).reshape(16, 2, 256)
    for o in range(2):
        ez[:, o, :, 0, o, :] = cz
        ez[:, o, :, 1, o, :] = sz
    ez_hi, ez_lo = np_split(ez.reshape(128, 512))
    inv_z = np.concatenate([ez_hi, ez_hi, ez_lo], 0)
    return dict(
        fwd_z=fwd_z, by=np.stack([by_hi, by_lo], 0), tw_y=tw_y, bx=bx, tw_x=tw_x, sel=sel,
        inv_x=inv_x, ey=np.stack([ey_hi, ey_lo], 0), tw_i=tw_i, inv_z=inv_z,
    )


def forward_z(advanced, fwd_z):
    hi, lo = split(advanced)
    return dot_nt(fwd_z, jnp.concatenate([hi, hi, lo], 1))


def forward_y(arrived, by_hi, by_lo, tw_c, tw_s):
    hi, lo = split(arrived)
    u = dot(jnp.concatenate([hi, lo], 0), by_hi)
    u = u[:128] + u[128:] + dot(hi, by_lo)
    real, imag = jnp.zeros((8, 256), F32), jnp.zeros((8, 256), F32)
    for c in range(N):
        ur, ui = u[8 * c:8 * c + 8, :256], u[8 * c:8 * c + 8, 256:]
        tc, ts = tw_c[c:c + 1, :], tw_s[c:c + 1, :]
        real += ur * tc + ui * ts
        imag += ui * tc - ur * ts
    return real, imag


def x_table(bx0, bx1, tc, ts):
    return split(bx0 * tc + bx1 * ts)


def forward_x(real, imag, bx_hi, bx_lo, roll):
    low = lax.broadcasted_iota(jnp.int32, (8, 128), 1) < 64
    rows = []
    for v in range(2):
        re, im = real[:, 128 * v:128 * v + 128], imag[:, 128 * v:128 * v + 128]
        rows.append(jnp.where(low, re, roll(im, 64, 1)))
        rows.append(jnp.where(low, roll(re, 64, 1), im))
    hi, lo = split(jnp.concatenate(rows, 0))
    u = dot(jnp.concatenate([hi, lo], 0), bx_hi)
    return u[:32] + u[32:] + dot(hi, bx_lo)


def lift_table(rows):
    i = lax.broadcasted_iota(jnp.int32, (32, 128), 0)
    lane = lax.broadcasted_iota(jnp.int32, (32, 128), 1)
    wide = dot_exact(rows, jnp.where(lane % 32 == i, 1.0, 0.0).astype(F32))
    upper = lax.broadcasted_iota(jnp.int32, (8, 128), 0) < 4
    return jnp.concatenate([jnp.where(upper, wide, 0.0), jnp.where(upper, 0.0, wide)], 1)


def local_table(rows, local_weight, local_bias):
    wide = jnp.concatenate([jnp.broadcast_to(rows[j:j + 1], (128, 32)) for j in range(4)], 0)
    scale = lax.dot_general(
        local_weight, wide, (((1,), (1,)), ((), ())), precision=lax.Precision.HIGHEST,
        preferred_element_type=F32)
    same = lax.broadcasted_iota(jnp.int32, (32, 32), 0) == lax.broadcasted_iota(
        jnp.int32, (32, 32), 1)
    bias = lax.dot_general(
        jnp.where(same, 1.0, 0.0).astype(F32), jnp.broadcast_to(local_bias, (128, 32)),
        (((1,), (1,)), ((), ())), precision=lax.Precision.HIGHEST, preferred_element_type=F32)
    return jnp.concatenate([scale[:, :384], scale[:, 384:] + bias], 1)


def lifted_coeffs(total, first, lift):
    row = lax.broadcasted_iota(jnp.int32, (8, 128), 0)
    lane = lax.broadcasted_iota(jnp.int32, (8, 128), 1)
    total = total * (1.0 / 8388608.0) + jnp.where((row == 3) & (lane == 0), first, 0.0)
    return dot_exact(total.T, lift)


def mix(coeffs, weight, sel):
    his, los = [], []
    for ky in range(2):
        for kz in range(2):
            cr = coeffs[64 * ky:64 * ky + 32, 128 * kz:128 * kz + 128]
            ci = coeffs[64 * ky + 32:64 * ky + 64, 128 * kz:128 * kz + 128]
            cr4 = jnp.concatenate([cr] * 4, 1)
            ci4 = jnp.concatenate([ci] * 4, 1)
            wr = weight(0, ky, kz).astype(F32)
            wi = weight(1, ky, kz).astype(F32)
            for value in (wr * cr4 - wi * ci4, wr * ci4 + wi * cr4):
                hi, lo = split(value)
                his.append(hi)
                los.append(lo)
    return dot(jnp.concatenate(his, 0), sel) + dot(jnp.concatenate(los, 0), sel)


def inverse_x(mixed, inv_x):
    lane = lax.broadcasted_iota(jnp.int32, (32, 128), 1)
    kind = lane % 4
    tops, bottoms = [], []
    for ky in range(2):
        block = [mixed[128 * ky + 32 * n:128 * ky + 32 * n + 32] for n in range(4)]

        def pick(a, b, c, d):
            return jnp.where(kind == 0, a, jnp.where(kind == 1, b, jnp.where(kind == 2, c, d)))

        tops.append(pick(block[0], block[1], block[2], block[3]))
        bottoms.append(pick(-block[1], block[0], -block[3], block[2]))
    top = jnp.where(lane < 64, tops[0], tops[1])
    bottom = jnp.where(lane < 64, bottoms[0], bottoms[1])
    hi, lo = split(jnp.concatenate([top, bottom], 0))
    return dot(inv_x, jnp.concatenate([hi, lo, hi], 0))


def turned(arrived, roll):
    even = lax.broadcasted_iota(jnp.int32, arrived.shape, 1) % 2 == 0
    other = jnp.where(even, roll(arrived, 127, 1), -roll(arrived, 1, 1))
    return [jnp.concatenate([t[:64], t[64:]], 1) for t in (arrived.T, other.T)]


def inverse_y(plain, other, tw_c, tw_s, ey_hi, ey_lo):
    his, los = [], []
    for m in range(8):
        tc, ts = tw_c[m:m + 1, :], tw_s[m:m + 1, :]
        hi, lo = split(jnp.concatenate([plain * tc - other * ts, other * tc + plain * ts], 1))
        his.append(hi)
        los.append(lo)
    hi, lo = jnp.concatenate(his, 0), jnp.concatenate(los, 0)
    return dot(hi, ey_hi) + dot(lo, ey_hi) + dot(hi, ey_lo)


def inverse_z(block, inv_z):
    hi, lo = split(block.T)
    return dot(jnp.concatenate([hi, lo, hi], 1), inv_z)


def activate(value):
    cubic = value * (0.7978845608028654 + 0.035677408136300125 * (value * value))
    half = 0.5 * value
    return half + half * jnp.tanh(cubic)


def ring(step, length):
    return min(step, length - step)


ROW_STEPS = sorted(
    ((a, b) for a in range(8) for b in range(2) if a or b), key=lambda s: (-ring(s[0], 8), s))
COL_STEPS = sorted(
    ((a, b) for a in range(4) for b in range(4) if a or b),
    key=lambda s: (-ring(s[0], 4) - ring(s[1], 4), s))
PIECES = ((0, 8), (8, 8), (16, 8), (24, 8))


def layer_kernel(*refs):
    hbm, refs = refs[:18], refs[18:]
    out_ref, refs = refs[0], refs[1:]
    here, refs = refs[:18], refs[18:]
    (step_ref, v_ref, t_ref, fz_ref, by_ref, twy_ref, bx_ref, twx_ref, lift_ref, bias_ref, lw_ref,
     lb_ref, w_ref, sel_ref, ix_ref, ey_ref, twi_ref, iz_ref) = here
    (adv_ref, local_ref, s1, r1, s2, r2, s3, r3, s4, g_ref, rows_ref,
     load_sem, send1, recv1, send2, recv2, send3, recv3, send4, recv4) = refs
    r = lax.axis_index("row")
    c = lax.axis_index("col")
    row_peers = [((r // 2 + a) % 8) * 2 + (r + b) % 2 for a, b in ROW_STEPS]
    col_peers = [((c // 4 + a) % 4) * 4 + (c + b) % 4 for a, b in COL_STEPS]

    loads = [
        pltpu.make_async_copy(src, dst, load_sem.at[n]) for n, (src, dst) in enumerate(zip(hbm, here))
    ]
    for load in loads[:4]:
        load.start()
    barrier = pltpu.get_barrier_semaphore()
    for peer in col_peers:
        pl.semaphore_signal(
            barrier, inc=1, device_id={"row": r, "col": peer}, device_id_type=MESH)
    for peer in row_peers:
        pl.semaphore_signal(
            barrier, inc=1, device_id={"row": peer, "col": c}, device_id_type=MESH)
    for load in loads[4:]:
        load.start()

    def to_col(src, dst, send, recv, peer):
        copy = pltpu.make_async_remote_copy(
            src_ref=src, dst_ref=dst, send_sem=send, recv_sem=recv,
            device_id={"row": r, "col": peer}, device_id_type=MESH)
        copy.start()
        return copy

    def to_row(src, dst, send, recv, peer):
        copy = pltpu.make_async_remote_copy(
            src_ref=src, dst_ref=dst, send_sem=send, recv_sem=recv,
            device_id={"row": peer, "col": c}, device_id_type=MESH)
        copy.start()
        return copy

    for load in loads[:4]:
        load.wait()
    advanced = v_ref[...] + step_ref[0] * t_ref[...]
    adv_ref[...] = advanced
    z = forward_z(advanced.reshape(384, 256), fz_ref[...])
    s1[pl.ds(3, 64, stride=4), :] = jnp.zeros((64, 128), F32)
    for j in range(3):
        s1[pl.ds(j, 64, stride=4), :] = z[:, 128 * j:128 * j + 128]
    pl.semaphore_wait(barrier, 2 * (N - 1))
    first = [
        to_col(s1.at[pl.ds(pl.multiple_of(16 * peer, 16), 16)], r1.at[c], send1.at[k], recv1.at[k],
               peer)
        for k, peer in enumerate(col_peers)
    ]
    r1[c] = s1[pl.ds(pl.multiple_of(16 * c, 16), 16), :]
    for load in loads[4:]:
        load.wait()
    bx_hi, bx_lo = x_table(
        bx_ref[0], bx_ref[1], twx_ref[0, pl.ds(r, 1), :], twx_ref[1, pl.ds(r, 1), :])
    for k in (0, 4):
        rows_ref[k:k + 3] = lift_ref[...]
        rows_ref[k + 3:k + 4] = bias_ref[...]
    lift = lift_table(rows_ref[...])
    local_ref[...] = local_table(rows_ref[...], lw_ref[...], lb_ref[...])
    for copy in first:
        copy.wait_recv()

    arrived = jnp.concatenate(
        [r1[:, 8 * part:8 * part + 8, :].reshape(128, 128) for part in range(2)], 1)
    real, imag = forward_y(arrived, by_ref[0], by_ref[1], twy_ref[0], twy_ref[1])
    partial = forward_x(real, imag, bx_hi, bx_lo, pltpu.roll)
    for g in range(4):
        for k in range(4):
            s2[4 * g + k] = partial[8 * g:8 * g + 8, 128 * k:128 * k + 128]
    second = [
        to_row(s2.at[peer], r2.at[r], send2.at[k], recv2.at[k], peer)
        for k, peer in enumerate(row_peers)
    ]
    r2[r] = s2[r]
    for copy in second:
        copy.wait_recv()
    total = jnp.sum(r2[...], axis=0)

    origin = jnp.where((r == 0) & (c == 0), 1.0, 0.0).astype(F32)
    coeffs = lifted_coeffs(total, origin, lift)
    third = []
    for half in range(2):
        mixed = mix(
            coeffs,
            lambda part, ky, kz: w_ref[part, ky, kz, :, 512 * half:512 * half + 512],
            sel_ref[...])
        s3[half] = inverse_x(mixed, ix_ref[...]).reshape(16, 8, 128)
        third.append([
            to_row(s3.at[half, peer], r3.at[half, r], send3.at[half, k], recv3.at[half, k], peer)
            for k, peer in enumerate(row_peers)
        ])
        r3[half, r] = s3[half, r]

    fourth = []
    for piece, (start, count) in enumerate(PIECES):
        if start % 16 == 0:
            half = start // 16
            for copy in third[half]:
                copy.wait_recv()
            plain, other = turned(r3[half].reshape(128, 128), pltpu.roll)
        rows = 4 * count
        first_row = 4 * (start % 16)
        h = inverse_y(
            plain[first_row:first_row + rows], other[first_row:first_row + rows],
            twi_ref[0], twi_ref[1], ey_ref[0], ey_ref[1])
        span = pl.ds(4 * start, rows)
        for dest in range(N):
            m, b = dest // 2, dest % 2
            s4[dest, span, :] = h[rows * m:rows * m + rows, 128 * b:128 * b + 128]
        fourth.append([
            to_col(s4.at[peer, span], g_ref.at[c, span], send4.at[piece, k], recv4.at[piece, k],
                   peer)
            for k, peer in enumerate(col_peers)
        ])
        g_ref[c, span, :] = s4[c, span, :]

    for piece, (start, count) in enumerate(PIECES):
        for copy in fourth[piece]:
            copy.wait_recv()
        for o in range(start, start + count, 2):
            values = inverse_z(g_ref[:, 4 * o:4 * o + 8, :].reshape(128, 128), iz_ref[...])
            for k in range(2):
                scale = [
                    jnp.concatenate([local_ref[o + k:o + k + 1, 128 * j:128 * j + 128]] * 2, 1)
                    for j in range(4)
                ]
                for x in range(8):
                    cell = slice(16 * x, 16 * x + 16)
                    value = values[cell, 256 * k:256 * k + 256] + scale[3]
                    for j in range(3):
                        value += scale[j] * adv_ref[j, cell, :]
                    out_ref[o + k, x] = activate(value).astype(BF16)
    for copies in [first, second] + third + fourth:
        for copy in copies:
            copy.wait_send()


def per_device(
    velocity, tendency, step_size, lift_weight, lift_bias, spectral_weight, local_weight, local_bias
):
    const = {name: jnp.asarray(a) for name, a in tables().items()}
    far = [
        step_size, velocity.reshape(3, 128, 256), tendency.reshape(3, 128, 256), const["fwd_z"],
        const["by"], const["tw_y"], const["bx"], const["tw_x"], lift_weight.T, lift_bias[None, :],
        local_weight, local_bias[None, :], spectral_weight, const["sel"], const["inv_x"],
        const["ey"], const["tw_i"], const["inv_z"],
    ]
    dma = pltpu.SemaphoreType.DMA
    out = pl.pallas_call(
        layer_kernel,
        out_shape=pltpu.VMEM((32, 8, 16, 256), BF16),
        in_specs=[pl.BlockSpec(memory_space=pl.ANY)] * len(far),
        out_specs=pl.BlockSpec(memory_space=pltpu.VMEM),
        scratch_shapes=[pltpu.SMEM((1,), F32)] + [pltpu.VMEM(a.shape, a.dtype) for a in far[1:]] + [
            pltpu.VMEM((3, 128, 256), F32), pltpu.VMEM((32, 512), F32),
            pltpu.VMEM((256, 128), F32), pltpu.VMEM((16, 16, 128), F32),
            pltpu.VMEM((16, 8, 128), F32), pltpu.VMEM((16, 8, 128), F32),
            pltpu.VMEM((2, 16, 8, 128), F32), pltpu.VMEM((2, 16, 8, 128), F32),
            pltpu.VMEM((16, 128, 128), F32), pltpu.VMEM((16, 128, 128), F32),
            pltpu.VMEM((8, 32), F32),
            dma((len(far),)), dma((N,)), dma((N,)), dma((N,)), dma((N,)),
            dma((2, N)), dma((2, N)), dma((len(PIECES), N)), dma((len(PIECES), N)),
        ],
        compiler_params=pltpu.CompilerParams(
            collective_id=0, has_side_effects=True, vmem_limit_bytes=VMEM_LIMIT),
        name="layer",
    )(*far)
    return out.reshape(1, 32, 8, 16, 256)


def solution(mesh):
    in_specs = (
        P(None, None, "row", "col", None),
        P(None, None, "row", "col", None),
        P(),
        P(),
        P(),
        P(None, "row", "col", None, None),
        P(),
        P(),
    )
    out_specs = P(None, None, "row", "col", None)
    return jax.shard_map(
        per_device, mesh=mesh, in_specs=in_specs, out_specs=out_specs, check_vma=False
    )
```

```python
import functools
import math

import jax
import jax.numpy as jnp
import numpy as np
from jax import lax
from jax.experimental import pallas as pl
from jax.experimental.pallas import tpu as pltpu
from jax.sharding import PartitionSpec as P

F32 = jnp.float32
BF16 = jnp.bfloat16
MESH = pl.DeviceIdType.MESH
VMEM_LIMIT = 60 * 1024 * 1024
N = 16


def split(x):
    hi = x.astype(BF16)
    lo = (x - hi.astype(F32)).astype(BF16)
    return hi, lo


def dot(a, b):
    return jnp.dot(a, b, preferred_element_type=F32)


def dot_nt(a, b):
    return lax.dot_general(a, b, (((1,), (1,)), ((), ())), preferred_element_type=F32)


def dot_exact(a, b):
    return jnp.dot(a, b, precision=lax.Precision.HIGHEST, preferred_element_type=F32)


def np_split(x):
    x = np.asarray(x, np.float64)
    hi = x.astype(np.float32).astype(jnp.bfloat16)
    lo = (x - hi.astype(np.float64)).astype(np.float32).astype(jnp.bfloat16)
    return hi, lo


@functools.lru_cache(None)
def tables():
    turn = 2.0 * np.pi
    ix = np.arange
    waves = np.where(ix(32) < 16, ix(32), ix(32) - 32)
    eye8 = np.eye(8)
    z_angle = turn * (ix(32)[:, None] * ix(256)[None, :] % 256) / 256
    z_hi, z_lo = np_split(np.concatenate([np.cos(z_angle), -np.sin(z_angle)], 0))
    fwd_z = np.concatenate([z_hi, z_lo, z_hi], 1)
    fwd_z = fwd_z.reshape(2, 16, 2, 768).transpose(1, 0, 2, 3).reshape(64, 768)
    a = turn * waves[None, :] * ix(16)[:, None] / 256
    by = np.zeros((2, 8, 16, 2, 32, 8))
    for x in range(8):
        by[0, x, :, 0, :, x] = np.cos(a)
        by[1, x, :, 0, :, x] = np.sin(a)
        by[0, x, :, 1, :, x] = -np.sin(a)
        by[1, x, :, 1, :, x] = np.cos(a)
    by_hi, by_lo = np_split(by.reshape(256, 512))
    b = turn * (waves[None, :] * ix(16)[:, None] % 16) / 16
    b = np.repeat(b, 8, axis=1)
    tw_y = np.stack([np.cos(b), np.sin(b)], 0).astype(np.float32)
    c = turn * waves[None, :] * ix(8)[:, None] / 128
    bx = []
    for quarter in (0.0, np.pi / 2):
        t = np.zeros((2, 8, 8, 8, 2, 32))
        for e in range(8):
            t[0, e, :, e, 0, :] = np.cos(c + quarter)
            t[1, e, :, e, 0, :] = np.sin(c + quarter)
            t[0, e, :, e, 1, :] = -np.sin(c + quarter)
            t[1, e, :, e, 1, :] = np.cos(c + quarter)
        bx.append(t.reshape(128, 512))
    bx = np.stack(bx, 0).astype(np.float32)
    d = turn * (waves[None, :] * ix(16)[:, None] % 16) / 16
    d = np.tile(d, (1, 16))
    tw_x = np.stack([np.cos(d), np.sin(d)], 0).astype(np.float32)
    sel = (ix(512)[:, None] // 32 == ix(128)[None, :] // 4 % 16).astype(jnp.bfloat16)
    f = turn * (waves[None, :] * ix(128)[:, None] % 128) / 128
    ex_hi, ex_lo = np_split(np.concatenate([np.cos(f), np.sin(f)], 1))
    inv_x = np.concatenate([ex_hi, ex_hi, ex_lo], 1)
    ey = []
    for apart in (1, 4):
        points = (apart * 16 * ix(2)[:, None] + ix(16)[None, :]).reshape(32)
        g = turn * (waves[:, None] * points[None, :] % 256) / 256
        t = np.zeros((2, 32, 8, 2, 8, 16))
        for x in range(8):
            for blk in range(2):
                t[0, :, x, blk, x, :] = np.cos(g[:, blk * 16:blk * 16 + 16])
                t[1, :, x, blk, x, :] = -np.sin(g[:, blk * 16:blk * 16 + 16])
        t = t.reshape(2, 16, 2, 8, 256).transpose(0, 2, 1, 3, 4)
        ey.extend(np_split(t.reshape(512, 256)))
    h = turn * (waves[None, :] * ix(16)[:, None] % 16) / 16
    h = np.repeat(h.reshape(16, 16, 2).transpose(0, 2, 1).reshape(16, 32), 8, axis=1)
    tw_i = np.stack([np.cos(h), np.sin(h)], 0).astype(np.float32)
    ez = np.zeros((16, 2, 2, 2, 2, 256))
    weight = np.where(ix(32) == 0, 1.0, 2.0)[:, None]
    cz = (weight * np.cos(z_angle)).reshape(16, 2, 256)
    sz = (-weight * np.sin(z_angle)).reshape(16, 2, 256)
    for o in range(2):
        ez[:, o, :, 0, o, :] = cz
        ez[:, o, :, 1, o, :] = sz
    ez_hi, ez_lo = np_split(ez.reshape(128, 512))
    inv_z = np.concatenate([ez_hi, ez_hi, ez_lo], 0)
    return dict(
        fwd_z=fwd_z, by=np.stack([by_hi, by_lo], 0), tw_y=tw_y, bx=bx, tw_x=tw_x, sel=sel,
        inv_x=inv_x, ey=np.stack(ey, 0), tw_i=tw_i, inv_z=inv_z,
    )


def forward_z(advanced, fwd_z):
    hi, lo = split(advanced)
    return dot_nt(fwd_z, jnp.concatenate([hi, hi, lo], 1))


def forward_y(arrived, by_hi, by_lo, tw_c, tw_s):
    hi, lo = split(arrived)
    u = dot(jnp.concatenate([hi, lo], 0), by_hi)
    u = u[:128] + u[128:] + dot(hi, by_lo)
    real, imag = jnp.zeros((8, 256), F32), jnp.zeros((8, 256), F32)
    for c in range(N):
        ur, ui = u[8 * c:8 * c + 8, :256], u[8 * c:8 * c + 8, 256:]
        tc, ts = tw_c[c:c + 1, :], tw_s[c:c + 1, :]
        real += ur * tc + ui * ts
        imag += ui * tc - ur * ts
    return real, imag


def x_table(bx0, bx1, tc, ts):
    return split(bx0 * tc + bx1 * ts)


def forward_x(real, imag, bx_hi, bx_lo, roll):
    low = lax.broadcasted_iota(jnp.int32, (8, 128), 1) < 64
    rows = []
    for v in range(2):
        re, im = real[:, 128 * v:128 * v + 128], imag[:, 128 * v:128 * v + 128]
        rows.append(jnp.where(low, re, roll(im, 64, 1)))
        rows.append(jnp.where(low, roll(re, 64, 1), im))
    hi, lo = split(jnp.concatenate(rows, 0))
    u = dot(jnp.concatenate([hi, lo], 0), bx_hi)
    return u[:32] + u[32:] + dot(hi, bx_lo)


def lift_table(rows):
    i = lax.broadcasted_iota(jnp.int32, (32, 128), 0)
    lane = lax.broadcasted_iota(jnp.int32, (32, 128), 1)
    wide = dot_exact(rows, jnp.where(lane % 32 == i, 1.0, 0.0).astype(F32))
    upper = lax.broadcasted_iota(jnp.int32, (8, 128), 0) < 4
    return jnp.concatenate([jnp.where(upper, wide, 0.0), jnp.where(upper, 0.0, wide)], 1)


def local_table(rows, local_weight, local_bias):
    wide = jnp.concatenate([jnp.broadcast_to(rows[j:j + 1], (128, 32)) for j in range(4)], 0)
    scale = lax.dot_general(
        local_weight, wide, (((1,), (1,)), ((), ())), precision=lax.Precision.HIGHEST,
        preferred_element_type=F32)
    same = lax.broadcasted_iota(jnp.int32, (32, 32), 0) == lax.broadcasted_iota(
        jnp.int32, (32, 32), 1)
    bias = lax.dot_general(
        jnp.where(same, 1.0, 0.0).astype(F32), jnp.broadcast_to(local_bias, (128, 32)),
        (((1,), (1,)), ((), ())), precision=lax.Precision.HIGHEST, preferred_element_type=F32)
    return jnp.concatenate([scale[:, :384], scale[:, 384:] + bias], 1)


def lifted_coeffs(total, first, lift):
    row = lax.broadcasted_iota(jnp.int32, (8, 128), 0)
    lane = lax.broadcasted_iota(jnp.int32, (8, 128), 1)
    total = total * (1.0 / 8388608.0) + jnp.where((row == 3) & (lane == 0), first, 0.0)
    return dot_exact(total.T, lift)


def mix(coeffs, weight, sel):
    his, los = [], []
    for ky in range(2):
        for kz in range(2):
            cr = coeffs[64 * ky:64 * ky + 32, 128 * kz:128 * kz + 128]
            ci = coeffs[64 * ky + 32:64 * ky + 64, 128 * kz:128 * kz + 128]
            cr4 = jnp.concatenate([cr] * 4, 1)
            ci4 = jnp.concatenate([ci] * 4, 1)
            wr = weight(0, ky, kz).astype(F32)
            wi = weight(1, ky, kz).astype(F32)
            for value in (wr * cr4 - wi * ci4, wr * ci4 + wi * cr4):
                hi, lo = split(value)
                his.append(hi)
                los.append(lo)
    return dot(jnp.concatenate(his, 0), sel) + dot(jnp.concatenate(los, 0), sel)


def inverse_x(mixed, inv_x):
    lane = lax.broadcasted_iota(jnp.int32, (32, 128), 1)
    kind = lane % 4
    tops, bottoms = [], []
    for ky in range(2):
        block = [mixed[128 * ky + 32 * n:128 * ky + 32 * n + 32] for n in range(4)]

        def pick(a, b, c, d):
            return jnp.where(kind == 0, a, jnp.where(kind == 1, b, jnp.where(kind == 2, c, d)))

        tops.append(pick(block[0], block[1], block[2], block[3]))
        bottoms.append(pick(-block[1], block[0], -block[3], block[2]))
    top = jnp.where(lane < 64, tops[0], tops[1])
    bottom = jnp.where(lane < 64, bottoms[0], bottoms[1])
    hi, lo = split(jnp.concatenate([top, bottom], 0))
    return dot(inv_x, jnp.concatenate([hi, lo, hi], 0))


def turned(arrived, roll):
    even = lax.broadcasted_iota(jnp.int32, arrived.shape, 1) % 2 == 0
    other = jnp.where(even, roll(arrived, 127, 1), -roll(arrived, 1, 1))
    return [jnp.concatenate([t[:64], t[64:]], 1) for t in (arrived.T, other.T)]


def swapped(plain):
    even = lax.broadcasted_iota(jnp.int32, plain.shape, 0) % 2 == 0
    rows = plain.shape[0]
    return jnp.where(even, pltpu.roll(plain, rows - 1, 0), -pltpu.roll(plain, 1, 0))


def inverse_y(plain, other, phases, ey_hi, ey_lo):
    his, los = [], []
    for tc, ts in phases:
        hi, lo = split(jnp.concatenate([plain * tc - other * ts, other * tc + plain * ts], 1))
        his.append(hi)
        los.append(lo)
    hi, lo = jnp.concatenate(his, 0), jnp.concatenate(los, 0)
    return dot(hi, ey_hi) + dot(lo, ey_hi) + dot(hi, ey_lo)


def inverse_z(block, inv_z):
    hi, lo = split(block.T)
    return dot(jnp.concatenate([hi, lo, hi], 1), inv_z)


def activate(value):
    cubic = value * (0.7978845608028654 + 0.035677408136300125 * (value * value))
    half = 0.5 * value
    return half + half * jnp.tanh(cubic)


def ring(step, length):
    return min(step, length - step)


ROW_STEPS = sorted(
    ((a, b) for a in range(8) for b in range(2) if a or b), key=lambda s: (-ring(s[0], 8), s))
COL_STEPS = sorted(
    ((a, b) for a in range(4) for b in range(4) if a or b),
    key=lambda s: (-ring(s[0], 4) - ring(s[1], 4), s))
PIECES = ((16, 8), (24, 8))


def layer_kernel(*refs):
    hbm, refs = refs[:18], refs[18:]
    out_ref, refs = refs[0], refs[1:]
    here, refs = refs[:18], refs[18:]
    (step_ref, v_ref, t_ref, fz_ref, by_ref, twy_ref, bx_ref, twx_ref, lift_ref, bias_ref, lw_ref,
     lb_ref, w_ref, sel_ref, ix_ref, ey_ref, twi_ref, iz_ref) = here
    (adv_ref, local_ref, s1, r1, s2, r2, s3, r3, s4, met, s5, g_ref, rows_ref,
     load_sem, send1, recv1, send2, recv2, send3, recv3, send4, recv4, send_m, recv_m, send5,
     recv5) = refs
    r = lax.axis_index("row")
    c = lax.axis_index("col")
    cy, cx = c // 4, c % 4
    row_peers = [((r // 2 + a) % 8) * 2 + (r + b) % 2 for a, b in ROW_STEPS]
    col_peers = [((c // 4 + a) % 4) * 4 + (c + b) % 4 for a, b in COL_STEPS]

    loads = [
        pltpu.make_async_copy(src, dst, load_sem.at[n]) for n, (src, dst) in enumerate(zip(hbm, here))
    ]
    for load in loads[:4]:
        load.start()
    barrier = pltpu.get_barrier_semaphore()
    for peer in col_peers:
        pl.semaphore_signal(
            barrier, inc=1, device_id={"row": r, "col": peer}, device_id_type=MESH)
    for peer in row_peers:
        pl.semaphore_signal(
            barrier, inc=1, device_id={"row": peer, "col": c}, device_id_type=MESH)
    for load in loads[4:]:
        load.start()

    def to_col(src, dst, send, recv, peer):
        copy = pltpu.make_async_remote_copy(
            src_ref=src, dst_ref=dst, send_sem=send, recv_sem=recv,
            device_id={"row": r, "col": peer}, device_id_type=MESH)
        copy.start()
        return copy

    def to_row(src, dst, send, recv, peer):
        copy = pltpu.make_async_remote_copy(
            src_ref=src, dst_ref=dst, send_sem=send, recv_sem=recv,
            device_id={"row": peer, "col": c}, device_id_type=MESH)
        copy.start()
        return copy

    for load in loads[:4]:
        load.wait()
    advanced = v_ref[...] + step_ref[0] * t_ref[...]
    adv_ref[...] = advanced
    z = forward_z(advanced.reshape(384, 256), fz_ref[...])
    s1[pl.ds(3, 64, stride=4), :] = jnp.zeros((64, 128), F32)
    for j in range(3):
        s1[pl.ds(j, 64, stride=4), :] = z[:, 128 * j:128 * j + 128]
    pl.semaphore_wait(barrier, 2 * (N - 1))
    first = [
        to_col(s1.at[pl.ds(pl.multiple_of(16 * peer, 16), 16)], r1.at[c], send1.at[k], recv1.at[k],
               peer)
        for k, peer in enumerate(col_peers)
    ]
    r1[c] = s1[pl.ds(pl.multiple_of(16 * c, 16), 16), :]
    for load in loads[4:]:
        load.wait()
    bx_hi, bx_lo = x_table(
        bx_ref[0], bx_ref[1], twx_ref[0, pl.ds(r, 1), :], twx_ref[1, pl.ds(r, 1), :])
    for k in (0, 4):
        rows_ref[k:k + 3] = lift_ref[...]
        rows_ref[k + 3:k + 4] = bias_ref[...]
    lift = lift_table(rows_ref[...])
    local_ref[...] = local_table(rows_ref[...], lw_ref[...], lb_ref[...])
    for copy in first:
        copy.wait_recv()

    arrived = jnp.concatenate(
        [r1[:, 8 * part:8 * part + 8, :].reshape(128, 128) for part in range(2)], 1)
    real, imag = forward_y(arrived, by_ref[0], by_ref[1], twy_ref[0], twy_ref[1])
    partial = forward_x(real, imag, bx_hi, bx_lo, pltpu.roll)
    for g in range(4):
        for k in range(4):
            s2[4 * g + k] = partial[8 * g:8 * g + 8, 128 * k:128 * k + 128]
    second = [
        to_row(s2.at[peer], r2.at[r], send2.at[k], recv2.at[k], peer)
        for k, peer in enumerate(row_peers)
    ]
    r2[r] = s2[r]
    for copy in second:
        copy.wait_recv()
    total = jnp.sum(r2[...], axis=0)

    origin = jnp.where((r == 0) & (c == 0), 1.0, 0.0).astype(F32)
    coeffs = lifted_coeffs(total, origin, lift)
    third = []
    for half in range(2):
        mixed = mix(
            coeffs,
            lambda part, ky, kz: w_ref[part, ky, kz, :, 512 * half:512 * half + 512],
            sel_ref[...])
        s3[half] = inverse_x(mixed, ix_ref[...]).reshape(16, 8, 128)
        third.append([
            to_row(s3.at[half, peer], r3.at[half, r], send3.at[half, k], recv3.at[half, k], peer)
            for k, peer in enumerate(row_peers)
        ])
        r3[half, r] = s3[half, r]

    def arrived_half(half):
        for copy in third[half]:
            copy.wait_recv()
        return turned(r3[half].reshape(128, 128), pltpu.roll)

    def phase(k):
        return twi_ref[0, pl.ds(k, 1), :], twi_ref[1, pl.ds(k, 1), :]

    plain, _ = arrived_half(0)
    met[0, cx] = plain[:32]
    met[1, cy] = plain[32:]
    meet = []
    for d in (2, 1, 3):
        meet.append(to_col(met.at[0, cx], met.at[0, cx], send_m.at[0, d], recv_m.at[0, d],
                           4 * cy + (cx + d) % 4))
        meet.append(to_col(met.at[1, cy], met.at[1, cy], send_m.at[1, d], recv_m.at[1, d],
                           4 * ((cy + d) % 4) + cx))

    plain, other = arrived_half(1)
    fourth = []
    for piece, (start, count) in enumerate(PIECES):
        rows = 4 * count
        near = slice(4 * (start - 16), 4 * (start - 16) + rows)
        h = inverse_y(plain[near], other[near], [phase(2 * m) for m in range(8)],
                      ey_ref[0], ey_ref[1])
        for dest in range(N):
            m, b = dest // 2, dest % 2
            s4[dest, near, :] = h[rows * m:rows * m + rows, 128 * b:128 * b + 128]
        span = pl.ds(4 * start, rows)
        fourth.append([
            to_col(s4.at[peer, pl.ds(near.start, rows)], g_ref.at[cy, cx, span],
                   send4.at[piece, k], recv4.at[piece, k], peer)
            for k, peer in enumerate(col_peers)
        ])
        g_ref[cy, cx, span, :] = s4[c, near, :]

    for copy in meet:
        copy.wait_recv()
    fifth = []
    for sub in range(2):
        fifth.append([])
        for axis in range(2):
            plain = met[axis, :, 16 * sub:16 * sub + 16, :].reshape(64, 256)
            phases = [phase(8 * m + cx) if axis == 0 else phase(4 * cy + 2 * m) for m in range(2)]
            table = 2 if axis == 0 else 0
            h = inverse_y(plain, swapped(plain), phases, ey_ref[table], ey_ref[table + 1])
            for t in range(4):
                m, b = t // 2, t % 2
                s5[axis, sub, t] = h[64 * m:64 * m + 64, 128 * b:128 * b + 128].reshape(4, 16, 128)
            span = pl.ds(32 * axis + 16 * sub, 16)
            for d in (2, 1, 3):
                sems = send5.at[axis, sub, d], recv5.at[axis, sub, d]
                if axis == 0:
                    t = (cy + d) % 4
                    fifth[sub].append(
                        to_col(s5.at[0, sub, t], g_ref.at[cy, :, span], *sems, 4 * t + cx))
                else:
                    t = (cx + d) % 4
                    fifth[sub].append(
                        to_col(s5.at[1, sub, t], g_ref.at[:, cx, span], *sems, 4 * cy + t))
            if axis == 0:
                g_ref[cy, :, span, :] = s5[0, sub, cy]
            else:
                g_ref[:, cx, span, :] = s5[1, sub, cx]

    def cells(start, count):
        for o in range(start, start + count, 2):
            values = inverse_z(g_ref[:, :, 4 * o:4 * o + 8, :].reshape(128, 128), iz_ref[...])
            for k in range(2):
                scale = [
                    jnp.concatenate([local_ref[o + k:o + k + 1, 128 * j:128 * j + 128]] * 2, 1)
                    for j in range(4)
                ]
                for x in range(8):
                    cell = slice(16 * x, 16 * x + 16)
                    value = values[cell, 256 * k:256 * k + 256] + scale[3]
                    for j in range(3):
                        value += scale[j] * adv_ref[j, cell, :]
                    out_ref[o + k, x] = activate(value).astype(BF16)

    for piece, (start, count) in enumerate(PIECES):
        for copy in fourth[piece]:
            copy.wait_recv()
        cells(start, count)
    for sub in range(2):
        for copy in fifth[sub]:
            copy.wait_recv()
        cells(4 * sub, 4)
        cells(8 + 4 * sub, 4)
    for copies in [first, second, meet] + third + fourth + fifth:
        for copy in copies:
            copy.wait_send()


def per_device(
    velocity, tendency, step_size, lift_weight, lift_bias, spectral_weight, local_weight, local_bias
):
    const = {name: jnp.asarray(a) for name, a in tables().items()}
    far = [
        step_size, velocity.reshape(3, 128, 256), tendency.reshape(3, 128, 256), const["fwd_z"],
        const["by"], const["tw_y"], const["bx"], const["tw_x"], lift_weight.T, lift_bias[None, :],
        local_weight, local_bias[None, :], spectral_weight, const["sel"], const["inv_x"],
        const["ey"], const["tw_i"], const["inv_z"],
    ]
    dma = pltpu.SemaphoreType.DMA
    out = pl.pallas_call(
        layer_kernel,
        out_shape=pltpu.VMEM((32, 8, 16, 256), BF16),
        in_specs=[pl.BlockSpec(memory_space=pl.ANY)] * len(far),
        out_specs=pl.BlockSpec(memory_space=pltpu.VMEM),
        scratch_shapes=[pltpu.SMEM((1,), F32)] + [pltpu.VMEM(a.shape, a.dtype) for a in far[1:]] + [
            pltpu.VMEM((3, 128, 256), F32), pltpu.VMEM((32, 512), F32),
            pltpu.VMEM((256, 128), F32), pltpu.VMEM((16, 16, 128), F32),
            pltpu.VMEM((16, 8, 128), F32), pltpu.VMEM((16, 8, 128), F32),
            pltpu.VMEM((2, 16, 8, 128), F32), pltpu.VMEM((2, 16, 8, 128), F32),
            pltpu.VMEM((16, 64, 128), F32), pltpu.VMEM((2, 4, 32, 256), F32),
            pltpu.VMEM((2, 2, 4, 4, 16, 128), F32), pltpu.VMEM((4, 4, 128, 128), F32),
            pltpu.VMEM((8, 32), F32),
            dma((len(far),)), dma((N,)), dma((N,)), dma((N,)), dma((N,)),
            dma((2, N)), dma((2, N)), dma((len(PIECES), N)), dma((len(PIECES), N)),
            dma((2, 4)), dma((2, 4)), dma((2, 2, 4)), dma((2, 2, 4)),
        ],
        compiler_params=pltpu.CompilerParams(
            collective_id=0, has_side_effects=True, vmem_limit_bytes=VMEM_LIMIT),
        name="layer",
    )(*far)
    return out.reshape(1, 32, 8, 16, 256)


def solution(mesh):
    in_specs = (
        P(None, None, "row", "col", None),
        P(None, None, "row", "col", None),
        P(),
        P(),
        P(),
        P(None, "row", "col", None, None),
        P(),
        P(),
    )
    out_specs = P(None, None, "row", "col", None)
    return jax.shard_map(
        per_device, mesh=mesh, in_specs=in_specs, out_specs=out_specs, check_vma=False
    )
```

```python
import functools
import math

import jax
import jax.numpy as jnp
import numpy as np
from jax import lax
from jax.experimental import pallas as pl
from jax.experimental.pallas import tpu as pltpu
from jax.sharding import PartitionSpec as P

F32 = jnp.float32
BF16 = jnp.bfloat16
MESH = pl.DeviceIdType.MESH
VMEM_LIMIT = 60 * 1024 * 1024
N = 16


def split(x):
    hi = x.astype(BF16)
    lo = (x - hi.astype(F32)).astype(BF16)
    return hi, lo


def dot(a, b):
    return jnp.dot(a, b, preferred_element_type=F32)


def dot_nt(a, b):
    return lax.dot_general(a, b, (((1,), (1,)), ((), ())), preferred_element_type=F32)


def dot_exact(a, b):
    return jnp.dot(a, b, precision=lax.Precision.HIGHEST, preferred_element_type=F32)


def np_split(x):
    x = np.asarray(x, np.float64)
    hi = x.astype(np.float32).astype(jnp.bfloat16)
    lo = (x - hi.astype(np.float64)).astype(np.float32).astype(jnp.bfloat16)
    return hi, lo


@functools.lru_cache(None)
def tables():
    turn = 2.0 * np.pi
    ix = np.arange
    waves = np.where(ix(32) < 16, ix(32), ix(32) - 32)
    eye8 = np.eye(8)
    z_angle = turn * (ix(32)[:, None] * ix(256)[None, :] % 256) / 256
    z_hi, z_lo = np_split(np.concatenate([np.cos(z_angle), -np.sin(z_angle)], 0))
    fwd_z = np.concatenate([z_hi, z_lo, z_hi], 1)
    fwd_z = fwd_z.reshape(2, 16, 2, 768).transpose(1, 0, 2, 3).reshape(64, 768)
    a = turn * waves[None, :] * ix(16)[:, None] / 256
    by = np.zeros((2, 8, 16, 2, 32, 8))
    for x in range(8):
        by[0, x, :, 0, :, x] = np.cos(a)
        by[1, x, :, 0, :, x] = np.sin(a)
        by[0, x, :, 1, :, x] = -np.sin(a)
        by[1, x, :, 1, :, x] = np.cos(a)
    by_hi, by_lo = np_split(by.reshape(256, 512))
    b = turn * (waves[None, :] * ix(16)[:, None] % 16) / 16
    b = np.repeat(b, 8, axis=1)
    tw_y = np.stack([np.cos(b), np.sin(b)], 0).astype(np.float32)
    c = turn * waves[None, :] * ix(8)[:, None] / 128
    bx = []
    for quarter in (0.0, np.pi / 2):
        t = np.zeros((2, 8, 8, 8, 2, 32))
        for e in range(8):
            t[0, e, :, e, 0, :] = np.cos(c + quarter)
            t[1, e, :, e, 0, :] = np.sin(c + quarter)
            t[0, e, :, e, 1, :] = -np.sin(c + quarter)
            t[1, e, :, e, 1, :] = np.cos(c + quarter)
        bx.append(t.reshape(128, 512))
    bx = np.stack(bx, 0).astype(np.float32)
    d = turn * (waves[None, :] * ix(16)[:, None] % 16) / 16
    d = np.tile(d, (1, 16))
    tw_x = np.stack([np.cos(d), np.sin(d)], 0).astype(np.float32)
    sel = (ix(512)[:, None] // 32 == ix(128)[None, :] // 4 % 16).astype(jnp.bfloat16)
    f = turn * (waves[None, :] * ix(128)[:, None] % 128) / 128
    ex_hi, ex_lo = np_split(np.concatenate([np.cos(f), np.sin(f)], 1))
    inv_x = np.concatenate([ex_hi, ex_hi, ex_lo], 1)
    ey = []
    for apart in (1, 4):
        points = (apart * 16 * ix(2)[:, None] + ix(16)[None, :]).reshape(32)
        g = turn * (waves[:, None] * points[None, :] % 256) / 256
        t = np.zeros((2, 32, 8, 2, 8, 16))
        for x in range(8):
            for blk in range(2):
                t[0, :, x, blk, x, :] = np.cos(g[:, blk * 16:blk * 16 + 16])
                t[1, :, x, blk, x, :] = -np.sin(g[:, blk * 16:blk * 16 + 16])
        t = t.reshape(2, 16, 2, 8, 256).transpose(0, 2, 1, 3, 4)
        ey.extend(np_split(t.reshape(512, 256)))
    h = turn * (waves[None, :] * ix(16)[:, None] % 16) / 16
    h = np.repeat(h.reshape(16, 16, 2).transpose(0, 2, 1).reshape(16, 32), 8, axis=1)
    tw_i = np.stack([np.cos(h), np.sin(h)], 0).astype(np.float32)
    ez = np.zeros((16, 2, 2, 2, 2, 256))
    weight = np.where(ix(32) == 0, 1.0, 2.0)[:, None]
    cz = (weight * np.cos(z_angle)).reshape(16, 2, 256)
    sz = (-weight * np.sin(z_angle)).reshape(16, 2, 256)
    for o in range(2):
        ez[:, o, :, 0, o, :] = cz
        ez[:, o, :, 1, o, :] = sz
    ez_hi, ez_lo = np_split(ez.reshape(128, 512))
    inv_z = np.concatenate([ez_hi, ez_hi, ez_lo], 0)
    return dict(
        fwd_z=fwd_z, by=np.stack([by_hi, by_lo], 0), tw_y=tw_y, bx=bx, tw_x=tw_x, sel=sel,
        inv_x=inv_x, ey=np.stack(ey, 0), tw_i=tw_i, inv_z=inv_z,
    )


def forward_z(advanced, fwd_z):
    hi, lo = split(advanced)
    return dot_nt(fwd_z, jnp.concatenate([hi, hi, lo], 1))


def forward_y(arrived, by_hi, by_lo, tw_c, tw_s):
    hi, lo = split(arrived)
    u = dot(jnp.concatenate([hi, lo], 0), by_hi)
    u = u[:128] + u[128:] + dot(hi, by_lo)
    real, imag = jnp.zeros((8, 256), F32), jnp.zeros((8, 256), F32)
    for c in range(N):
        ur, ui = u[8 * c:8 * c + 8, :256], u[8 * c:8 * c + 8, 256:]
        tc, ts = tw_c[c:c + 1, :], tw_s[c:c + 1, :]
        real += ur * tc + ui * ts
        imag += ui * tc - ur * ts
    return real, imag


def x_table(bx0, bx1, tc, ts):
    return split(bx0 * tc + bx1 * ts)


def forward_x(real, imag, bx_hi, bx_lo, roll):
    low = lax.broadcasted_iota(jnp.int32, (8, 128), 1) < 64
    rows = []
    for v in range(2):
        re, im = real[:, 128 * v:128 * v + 128], imag[:, 128 * v:128 * v + 128]
        rows.append(jnp.where(low, re, roll(im, 64, 1)))
        rows.append(jnp.where(low, roll(re, 64, 1), im))
    hi, lo = split(jnp.concatenate(rows, 0))
    u = dot(jnp.concatenate([hi, lo], 0), bx_hi)
    return u[:32] + u[32:] + dot(hi, bx_lo)


def lift_table(rows):
    i = lax.broadcasted_iota(jnp.int32, (32, 128), 0)
    lane = lax.broadcasted_iota(jnp.int32, (32, 128), 1)
    wide = dot_exact(rows, jnp.where(lane % 32 == i, 1.0, 0.0).astype(F32))
    upper = lax.broadcasted_iota(jnp.int32, (8, 128), 0) < 4
    return jnp.concatenate([jnp.where(upper, wide, 0.0), jnp.where(upper, 0.0, wide)], 1)


def local_table(rows, local_weight, local_bias):
    wide = jnp.concatenate([jnp.broadcast_to(rows[j:j + 1], (128, 32)) for j in range(4)], 0)
    scale = lax.dot_general(
        local_weight, wide, (((1,), (1,)), ((), ())), precision=lax.Precision.HIGHEST,
        preferred_element_type=F32)
    same = lax.broadcasted_iota(jnp.int32, (32, 32), 0) == lax.broadcasted_iota(
        jnp.int32, (32, 32), 1)
    bias = lax.dot_general(
        jnp.where(same, 1.0, 0.0).astype(F32), jnp.broadcast_to(local_bias, (128, 32)),
        (((1,), (1,)), ((), ())), precision=lax.Precision.HIGHEST, preferred_element_type=F32)
    return jnp.concatenate([scale[:, :384], scale[:, 384:] + bias], 1)


def lifted_coeffs(total, first, lift):
    row = lax.broadcasted_iota(jnp.int32, (8, 128), 0)
    lane = lax.broadcasted_iota(jnp.int32, (8, 128), 1)
    total = total * (1.0 / 8388608.0) + jnp.where((row == 3) & (lane == 0), first, 0.0)
    return dot_exact(total.T, lift)


def mix(coeffs, weight, sel):
    his, los = [], []
    for ky in range(2):
        for kz in range(2):
            cr = coeffs[64 * ky:64 * ky + 32, 128 * kz:128 * kz + 128]
            ci = coeffs[64 * ky + 32:64 * ky + 64, 128 * kz:128 * kz + 128]
            cr4 = jnp.concatenate([cr] * 4, 1)
            ci4 = jnp.concatenate([ci] * 4, 1)
            wr = weight(0, ky, kz).astype(F32)
            wi = weight(1, ky, kz).astype(F32)
            for value in (wr * cr4 - wi * ci4, wr * ci4 + wi * cr4):
                hi, lo = split(value)
                his.append(hi)
                los.append(lo)
    return dot(jnp.concatenate(his, 0), sel) + dot(jnp.concatenate(los, 0), sel)


def inverse_x(mixed, inv_x):
    lane = lax.broadcasted_iota(jnp.int32, (32, 128), 1)
    kind = lane % 4
    tops, bottoms = [], []
    for ky in range(2):
        block = [mixed[128 * ky + 32 * n:128 * ky + 32 * n + 32] for n in range(4)]

        def pick(a, b, c, d):
            return jnp.where(kind == 0, a, jnp.where(kind == 1, b, jnp.where(kind == 2, c, d)))

        tops.append(pick(block[0], block[1], block[2], block[3]))
        bottoms.append(pick(-block[1], block[0], -block[3], block[2]))
    top = jnp.where(lane < 64, tops[0], tops[1])
    bottom = jnp.where(lane < 64, bottoms[0], bottoms[1])
    hi, lo = split(jnp.concatenate([top, bottom], 0))
    return dot(inv_x, jnp.concatenate([hi, lo, hi], 0))


def turned(arrived, roll):
    even = lax.broadcasted_iota(jnp.int32, arrived.shape, 1) % 2 == 0
    other = jnp.where(even, roll(arrived, 127, 1), -roll(arrived, 1, 1))
    return [jnp.concatenate([t[:64], t[64:]], 1) for t in (arrived.T, other.T)]


def swapped(plain):
    even = lax.broadcasted_iota(jnp.int32, plain.shape, 0) % 2 == 0
    rows = plain.shape[0]
    return jnp.where(even, pltpu.roll(plain, rows - 1, 0), -pltpu.roll(plain, 1, 0))


def inverse_y(plain, other, phases, ey_hi, ey_lo):
    his, los = [], []
    for tc, ts in phases:
        hi, lo = split(jnp.concatenate([plain * tc - other * ts, other * tc + plain * ts], 1))
        his.append(hi)
        los.append(lo)
    hi, lo = jnp.concatenate(his, 0), jnp.concatenate(los, 0)
    return dot(hi, ey_hi) + dot(lo, ey_hi) + dot(hi, ey_lo)


def inverse_z(block, inv_z):
    hi, lo = split(block.T)
    return dot(jnp.concatenate([hi, lo, hi], 1), inv_z)


def activate(value):
    cubic = value * (0.7978845608028654 + 0.035677408136300125 * (value * value))
    half = 0.5 * value
    return half + half * jnp.tanh(cubic)


def ring(step, length):
    return min(step, length - step)


ROW_STEPS = sorted(
    ((a, b) for a in range(8) for b in range(2) if a or b), key=lambda s: (-ring(s[0], 8), s))
COL_STEPS = sorted(
    ((a, b) for a in range(4) for b in range(4) if a or b),
    key=lambda s: (-ring(s[0], 4) - ring(s[1], 4), s))
PIECES = ((16, 8),)
MEETS = ((0, 8, 8, (4, 4)), (24, 28, 4, (2, 2)))


def layer_kernel(*refs):
    hbm, refs = refs[:18], refs[18:]
    out_ref, refs = refs[0], refs[1:]
    here, refs = refs[:18], refs[18:]
    (step_ref, v_ref, t_ref, fz_ref, by_ref, twy_ref, bx_ref, twx_ref, lift_ref, bias_ref, lw_ref,
     lb_ref, w_ref, sel_ref, ix_ref, ey_ref, twi_ref, iz_ref) = here
    (adv_ref, local_ref, s1, r1, s2, r2, s3, r3, s4, met, s5, g_ref, rows_ref,
     load_sem, send1, recv1, send2, recv2, send3, recv3, send4, recv4, send_m, recv_m, send5,
     recv5) = refs
    r = lax.axis_index("row")
    c = lax.axis_index("col")
    cy, cx = c // 4, c % 4
    row_peers = [((r // 2 + a) % 8) * 2 + (r + b) % 2 for a, b in ROW_STEPS]
    col_peers = [((c // 4 + a) % 4) * 4 + (c + b) % 4 for a, b in COL_STEPS]

    loads = [
        pltpu.make_async_copy(src, dst, load_sem.at[n]) for n, (src, dst) in enumerate(zip(hbm, here))
    ]
    for load in loads[:4]:
        load.start()
    barrier = pltpu.get_barrier_semaphore()
    for peer in col_peers:
        pl.semaphore_signal(
            barrier, inc=1, device_id={"row": r, "col": peer}, device_id_type=MESH)
    for peer in row_peers:
        pl.semaphore_signal(
            barrier, inc=1, device_id={"row": peer, "col": c}, device_id_type=MESH)
    for load in loads[4:]:
        load.start()

    def to_col(src, dst, send, recv, peer):
        copy = pltpu.make_async_remote_copy(
            src_ref=src, dst_ref=dst, send_sem=send, recv_sem=recv,
            device_id={"row": r, "col": peer}, device_id_type=MESH)
        copy.start()
        return copy

    def to_row(src, dst, send, recv, peer):
        copy = pltpu.make_async_remote_copy(
            src_ref=src, dst_ref=dst, send_sem=send, recv_sem=recv,
            device_id={"row": peer, "col": c}, device_id_type=MESH)
        copy.start()
        return copy

    for load in loads[:4]:
        load.wait()
    advanced = v_ref[...] + step_ref[0] * t_ref[...]
    adv_ref[...] = advanced
    z = forward_z(advanced.reshape(384, 256), fz_ref[...])
    s1[pl.ds(3, 64, stride=4), :] = jnp.zeros((64, 128), F32)
    for j in range(3):
        s1[pl.ds(j, 64, stride=4), :] = z[:, 128 * j:128 * j + 128]
    pl.semaphore_wait(barrier, 2 * (N - 1))
    first = [
        to_col(s1.at[pl.ds(pl.multiple_of(16 * peer, 16), 16)], r1.at[c], send1.at[k], recv1.at[k],
               peer)
        for k, peer in enumerate(col_peers)
    ]
    r1[c] = s1[pl.ds(pl.multiple_of(16 * c, 16), 16), :]
    for load in loads[4:]:
        load.wait()
    bx_hi, bx_lo = x_table(
        bx_ref[0], bx_ref[1], twx_ref[0, pl.ds(r, 1), :], twx_ref[1, pl.ds(r, 1), :])
    for k in (0, 4):
        rows_ref[k:k + 3] = lift_ref[...]
        rows_ref[k + 3:k + 4] = bias_ref[...]
    lift = lift_table(rows_ref[...])
    local_ref[...] = local_table(rows_ref[...], lw_ref[...], lb_ref[...])
    for copy in first:
        copy.wait_recv()

    arrived = jnp.concatenate(
        [r1[:, 8 * part:8 * part + 8, :].reshape(128, 128) for part in range(2)], 1)
    real, imag = forward_y(arrived, by_ref[0], by_ref[1], twy_ref[0], twy_ref[1])
    partial = forward_x(real, imag, bx_hi, bx_lo, pltpu.roll)
    for g in range(4):
        for k in range(4):
            s2[4 * g + k] = partial[8 * g:8 * g + 8, 128 * k:128 * k + 128]
    second = [
        to_row(s2.at[peer], r2.at[r], send2.at[k], recv2.at[k], peer)
        for k, peer in enumerate(row_peers)
    ]
    r2[r] = s2[r]
    for copy in second:
        copy.wait_recv()
    total = jnp.sum(r2[...], axis=0)

    origin = jnp.where((r == 0) & (c == 0), 1.0, 0.0).astype(F32)
    coeffs = lifted_coeffs(total, origin, lift)
    third = []
    for half in range(2):
        mixed = mix(
            coeffs,
            lambda part, ky, kz: w_ref[part, ky, kz, :, 512 * half:512 * half + 512],
            sel_ref[...])
        s3[half] = inverse_x(mixed, ix_ref[...]).reshape(16, 8, 128)
        third.append([
            to_row(s3.at[half, peer], r3.at[half, r], send3.at[half, k], recv3.at[half, k], peer)
            for k, peer in enumerate(row_peers)
        ])
        r3[half, r] = s3[half, r]

    def arrived_half(half):
        for copy in third[half]:
            copy.wait_recv()
        return turned(r3[half].reshape(128, 128), pltpu.roll)

    def phase(k):
        return twi_ref[0, pl.ds(k, 1), :], twi_ref[1, pl.ds(k, 1), :]

    def meet(entry, plain):
        copies = []
        for axis in range(2):
            start, count = MEETS[entry][axis], MEETS[entry][2]
            first_row = 4 * (start % 16)
            place = met.at[axis, cx if axis == 0 else cy, pl.ds(32 * entry, 4 * count)]
            place[...] = plain[first_row:first_row + 4 * count]
            for d in (2, 1, 3):
                peer = 4 * cy + (cx + d) % 4 if axis == 0 else 4 * ((cy + d) % 4) + cx
                copies.append(to_col(
                    place, place, send_m.at[entry, axis, d], recv_m.at[entry, axis, d], peer))
        return copies

    plain, _ = arrived_half(0)
    meets = [meet(0, plain)]
    plain, other = arrived_half(1)
    meets.append(meet(1, plain))
    fourth = []
    for piece, (start, count) in enumerate(PIECES):
        rows = 4 * count
        near = slice(4 * (start - 16), 4 * (start - 16) + rows)
        h = inverse_y(plain[near], other[near], [phase(2 * m) for m in range(8)],
                      ey_ref[0], ey_ref[1])
        for dest in range(N):
            m, b = dest // 2, dest % 2
            s4[dest, near, :] = h[rows * m:rows * m + rows, 128 * b:128 * b + 128]
        span = pl.ds(4 * start, rows)
        fourth.append([
            to_col(s4.at[peer, pl.ds(near.start, rows)], g_ref.at[cy, cx, span],
                   send4.at[piece, k], recv4.at[piece, k], peer)
            for k, peer in enumerate(col_peers)
        ])
        g_ref[cy, cx, span, :] = s4[c, near, :]

    fifth = []
    for entry, (start_x, start_y, _, parts) in enumerate(MEETS):
        for copy in meets[entry]:
            copy.wait_recv()
        done = 0
        for count in parts:
            part = len(fifth)
            rows = 4 * count
            copies = []
            for axis, start in enumerate((start_x, start_y)):
                far = pl.ds(32 * entry + 4 * done, rows)
                plain = met[axis, :, far, :].reshape(4 * rows, 256)
                phases = [
                    phase(8 * m + cx) if axis == 0 else phase(4 * cy + 2 * m) for m in range(2)]
                table = 2 if axis == 0 else 0
                h = inverse_y(plain, swapped(plain), phases, ey_ref[table], ey_ref[table + 1])
                for t in range(4):
                    m, b = t // 2, t % 2
                    s5[part, axis, t, :, :rows] = h[
                        4 * rows * m:4 * rows * m + 4 * rows, 128 * b:128 * b + 128
                    ].reshape(4, rows, 128)
                span = pl.ds(4 * (start + done), rows)
                for d in (2, 1, 3):
                    sems = send5.at[part, axis, d], recv5.at[part, axis, d]
                    if axis == 0:
                        t = (cy + d) % 4
                        copies.append(
                            to_col(s5.at[part, 0, t, :, pl.ds(0, rows)], g_ref.at[cy, :, span], *sems, 4 * t + cx))
                    else:
                        t = (cx + d) % 4
                        copies.append(
                            to_col(s5.at[part, 1, t, :, pl.ds(0, rows)], g_ref.at[:, cx, span], *sems, 4 * cy + t))
                if axis == 0:
                    g_ref[cy, :, span, :] = s5[part, 0, cy, :, :rows]
                else:
                    g_ref[:, cx, span, :] = s5[part, 1, cx, :, :rows]
            fifth.append((copies, start_x + done, start_y + done, count))
            done += count

    def cells(start, count):
        for o in range(start, start + count, 2):
            values = inverse_z(g_ref[:, :, 4 * o:4 * o + 8, :].reshape(128, 128), iz_ref[...])
            for k in range(2):
                scale = [
                    jnp.concatenate([local_ref[o + k:o + k + 1, 128 * j:128 * j + 128]] * 2, 1)
                    for j in range(4)
                ]
                for x in range(8):
                    cell = slice(16 * x, 16 * x + 16)
                    value = values[cell, 256 * k:256 * k + 256] + scale[3]
                    for j in range(3):
                        value += scale[j] * adv_ref[j, cell, :]
                    out_ref[o + k, x] = activate(value).astype(BF16)

    for piece, (start, count) in enumerate(PIECES):
        for copy in fourth[piece]:
            copy.wait_recv()
        cells(start, count)
    for copies, start_x, start_y, count in fifth:
        for copy in copies:
            copy.wait_recv()
        cells(start_x, count)
        cells(start_y, count)
    for copies in [first, second] + third + meets + fourth + [entry[0] for entry in fifth]:
        for copy in copies:
            copy.wait_send()


def per_device(
    velocity, tendency, step_size, lift_weight, lift_bias, spectral_weight, local_weight, local_bias
):
    const = {name: jnp.asarray(a) for name, a in tables().items()}
    far = [
        step_size, velocity.reshape(3, 128, 256), tendency.reshape(3, 128, 256), const["fwd_z"],
        const["by"], const["tw_y"], const["bx"], const["tw_x"], lift_weight.T, lift_bias[None, :],
        local_weight, local_bias[None, :], spectral_weight, const["sel"], const["inv_x"],
        const["ey"], const["tw_i"], const["inv_z"],
    ]
    dma = pltpu.SemaphoreType.DMA
    out = pl.pallas_call(
        layer_kernel,
        out_shape=pltpu.VMEM((32, 8, 16, 256), BF16),
        in_specs=[pl.BlockSpec(memory_space=pl.ANY)] * len(far),
        out_specs=pl.BlockSpec(memory_space=pltpu.VMEM),
        scratch_shapes=[pltpu.SMEM((1,), F32)] + [pltpu.VMEM(a.shape, a.dtype) for a in far[1:]] + [
            pltpu.VMEM((3, 128, 256), F32), pltpu.VMEM((32, 512), F32),
            pltpu.VMEM((256, 128), F32), pltpu.VMEM((16, 16, 128), F32),
            pltpu.VMEM((16, 8, 128), F32), pltpu.VMEM((16, 8, 128), F32),
            pltpu.VMEM((2, 16, 8, 128), F32), pltpu.VMEM((2, 16, 8, 128), F32),
            pltpu.VMEM((16, 64, 128), F32), pltpu.VMEM((2, 4, 64, 256), F32),
            pltpu.VMEM((4, 2, 4, 4, 16, 128), F32), pltpu.VMEM((4, 4, 128, 128), F32),
            pltpu.VMEM((8, 32), F32),
            dma((len(far),)), dma((N,)), dma((N,)), dma((N,)), dma((N,)),
            dma((2, N)), dma((2, N)), dma((len(PIECES), N)), dma((len(PIECES), N)),
            dma((2, 2, 4)), dma((2, 2, 4)), dma((4, 2, 4)), dma((4, 2, 4)),
        ],
        compiler_params=pltpu.CompilerParams(
            collective_id=0, has_side_effects=True, vmem_limit_bytes=VMEM_LIMIT),
        name="layer",
    )(*far)
    return out.reshape(1, 32, 8, 16, 256)


def solution(mesh):
    in_specs = (
        P(None, None, "row", "col", None),
        P(None, None, "row", "col", None),
        P(),
        P(),
        P(),
        P(None, "row", "col", None, None),
        P(),
        P(),
    )
    out_specs = P(None, None, "row", "col", None)
    return jax.shard_map(
        per_device, mesh=mesh, in_specs=in_specs, out_specs=out_specs, check_vma=False
    )
```

```python
import functools
import math

import jax
import jax.numpy as jnp
import numpy as np
from jax import lax
from jax.experimental import pallas as pl
from jax.experimental.pallas import tpu as pltpu
from jax.sharding import PartitionSpec as P

F32 = jnp.float32
BF16 = jnp.bfloat16
MESH = pl.DeviceIdType.MESH
VMEM_LIMIT = 60 * 1024 * 1024
N = 16


def split(x):
    hi = x.astype(BF16)
    lo = (x - hi.astype(F32)).astype(BF16)
    return hi, lo


def dot(a, b):
    return jnp.dot(a, b, preferred_element_type=F32)


def dot_nt(a, b):
    return lax.dot_general(a, b, (((1,), (1,)), ((), ())), preferred_element_type=F32)


def dot_exact(a, b):
    return jnp.dot(a, b, precision=lax.Precision.HIGHEST, preferred_element_type=F32)


def np_split(x):
    x = np.asarray(x, np.float64)
    hi = x.astype(np.float32).astype(jnp.bfloat16)
    lo = (x - hi.astype(np.float64)).astype(np.float32).astype(jnp.bfloat16)
    return hi, lo


@functools.lru_cache(None)
def tables():
    turn = 2.0 * np.pi
    ix = np.arange
    waves = np.where(ix(32) < 16, ix(32), ix(32) - 32)
    eye8 = np.eye(8)
    z_angle = turn * (ix(32)[:, None] * ix(256)[None, :] % 256) / 256
    z_hi, z_lo = np_split(np.concatenate([np.cos(z_angle), -np.sin(z_angle)], 0))
    fwd_z = np.concatenate([z_hi, z_lo, z_hi], 1)
    fwd_z = fwd_z.reshape(2, 16, 2, 768).transpose(1, 0, 2, 3).reshape(64, 768)
    a = turn * waves[None, :] * ix(16)[:, None] / 256
    by = np.zeros((2, 8, 16, 2, 32, 8))
    for x in range(8):
        by[0, x, :, 0, :, x] = np.cos(a)
        by[1, x, :, 0, :, x] = np.sin(a)
        by[0, x, :, 1, :, x] = -np.sin(a)
        by[1, x, :, 1, :, x] = np.cos(a)
    by_hi, by_lo = np_split(by.reshape(256, 512))
    b = turn * (waves[None, :] * ix(16)[:, None] % 16) / 16
    b = np.repeat(b, 8, axis=1)
    tw_y = np.stack([np.cos(b), np.sin(b)], 0).astype(np.float32)
    c = turn * waves[None, :] * ix(8)[:, None] / 128
    bx = []
    for quarter in (0.0, np.pi / 2):
        t = np.zeros((2, 8, 8, 8, 2, 32))
        for e in range(8):
            t[0, e, :, e, 0, :] = np.cos(c + quarter)
            t[1, e, :, e, 0, :] = np.sin(c + quarter)
            t[0, e, :, e, 1, :] = -np.sin(c + quarter)
            t[1, e, :, e, 1, :] = np.cos(c + quarter)
        bx.append(t.reshape(128, 512))
    bx = np.stack(bx, 0).astype(np.float32)
    d = turn * (waves[None, :] * ix(16)[:, None] % 16) / 16
    d = np.tile(d, (1, 16))
    tw_x = np.stack([np.cos(d), np.sin(d)], 0).astype(np.float32)
    f = turn * (waves[None, :] * ix(128)[:, None] % 128) / 128
    ex_hi, ex_lo = np_split(np.concatenate([np.cos(f), np.sin(f)], 1))
    inv_x = np.concatenate([ex_hi, ex_hi, ex_lo], 1)
    ey = []
    for apart in (1, 4):
        points = (apart * 16 * ix(2)[:, None] + ix(16)[None, :]).reshape(32)
        g = turn * (waves[:, None] * points[None, :] % 256) / 256
        t = np.zeros((2, 32, 8, 2, 8, 16))
        for x in range(8):
            for blk in range(2):
                t[0, :, x, blk, x, :] = np.cos(g[:, blk * 16:blk * 16 + 16])
                t[1, :, x, blk, x, :] = -np.sin(g[:, blk * 16:blk * 16 + 16])
        t = t.reshape(2, 16, 2, 8, 256).transpose(0, 2, 1, 3, 4)
        ey.extend(np_split(t.reshape(512, 256)))
    h = turn * (waves[None, :] * ix(16)[:, None] % 16) / 16
    h = np.repeat(h.reshape(16, 16, 2).transpose(0, 2, 1).reshape(16, 32), 8, axis=1)
    tw_i = np.stack([np.cos(h), np.sin(h)], 0).astype(np.float32)
    ez = np.zeros((16, 2, 2, 2, 2, 256))
    weight = np.where(ix(32) == 0, 1.0, 2.0)[:, None]
    cz = (weight * np.cos(z_angle)).reshape(16, 2, 256)
    sz = (-weight * np.sin(z_angle)).reshape(16, 2, 256)
    for o in range(2):
        ez[:, o, :, 0, o, :] = cz
        ez[:, o, :, 1, o, :] = sz
    ez_hi, ez_lo = np_split(ez.reshape(128, 512))
    inv_z = np.concatenate([ez_hi, ez_hi, ez_lo], 0)
    return dict(
        fwd_z=fwd_z, by=np.stack([by_hi, by_lo], 0), tw_y=tw_y, bx=bx, tw_x=tw_x,
        inv_x=inv_x, ey=np.stack(ey, 0), tw_i=tw_i, inv_z=inv_z,
    )


def forward_z(advanced, fwd_z):
    hi, lo = split(advanced)
    return dot_nt(fwd_z, jnp.concatenate([hi, hi, lo], 1))


def forward_y(arrived, by_hi, by_lo, tw_c, tw_s):
    hi, lo = split(arrived)
    u = dot(jnp.concatenate([hi, lo], 0), by_hi)
    u = u[:128] + u[128:] + dot(hi, by_lo)
    real, imag = jnp.zeros((8, 256), F32), jnp.zeros((8, 256), F32)
    for c in range(N):
        ur, ui = u[8 * c:8 * c + 8, :256], u[8 * c:8 * c + 8, 256:]
        tc, ts = tw_c[c:c + 1, :], tw_s[c:c + 1, :]
        real += ur * tc + ui * ts
        imag += ui * tc - ur * ts
    return real, imag


def x_table(bx0, bx1, tc, ts):
    return split(bx0 * tc + bx1 * ts)


def forward_x(real, imag, bx_hi, bx_lo, roll):
    low = lax.broadcasted_iota(jnp.int32, (8, 128), 1) < 64
    rows = []
    for v in range(2):
        re, im = real[:, 128 * v:128 * v + 128], imag[:, 128 * v:128 * v + 128]
        rows.append(jnp.where(low, re, roll(im, 64, 1)))
        rows.append(jnp.where(low, roll(re, 64, 1), im))
    hi, lo = split(jnp.concatenate(rows, 0))
    u = dot(jnp.concatenate([hi, lo], 0), bx_hi)
    return u[:32] + u[32:] + dot(hi, bx_lo)


def dot_nt_exact(a, b):
    return lax.dot_general(
        a, b, (((1,), (1,)), ((), ())), precision=lax.Precision.HIGHEST, preferred_element_type=F32)


def spread(rows):
    return jnp.concatenate([jnp.broadcast_to(rows[j:j + 1], (128, 32)) for j in range(4)], 0)


def identity():
    return jnp.where(
        lax.broadcasted_iota(jnp.int32, (32, 32), 0) == lax.broadcasted_iota(
            jnp.int32, (32, 32), 1), 1.0, 0.0).astype(F32)


def local_table(rows, local_weight, local_bias):
    scale = dot_nt_exact(local_weight, spread(rows))
    bias = dot_nt_exact(identity(), jnp.broadcast_to(local_bias, (128, 32)))
    return jnp.concatenate([scale[:, :384], scale[:, 384:] + bias], 1)


def lane(shape):
    return lax.broadcasted_iota(jnp.int32, shape, len(shape) - 1)


def lift_tables(rows):
    columns = dot_nt_exact(identity(), spread(rows))
    own = lax.broadcasted_iota(jnp.int32, (512, 128), 0) // 32 == lane((512, 128)) // 4 % 16
    return [
        split(jnp.where(own, jnp.concatenate([columns[:, 128 * j:128 * j + 128]] * 16, 0), 0.0))
        for j in range(4)
    ]


def lifted_weights(blocks, lift):
    stacked = jnp.concatenate([b for part in blocks for row in part for b in row], 0)
    u = dot(stacked, lift[0]) + dot(stacked, lift[1])
    first_kz, first_ky = lane((32, 128)) % 4 < 2, lane((32, 128)) < 64
    out = []
    for part in range(2):
        b = [u[128 * part + 32 * n:128 * part + 32 * n + 32] for n in range(4)]
        out.append(jnp.where(
            first_ky, jnp.where(first_kz, b[0], b[1]), jnp.where(first_kz, b[2], b[3])))
    return out


def spread_modes(total, first):
    row, column = lax.broadcasted_iota(jnp.int32, (8, 128), 0), lane((8, 128))
    total = total * (1.0 / 8388608.0) + jnp.where((row == 3) & (column == 0), first, 0.0)
    row, column = lax.broadcasted_iota(jnp.int32, (8, 512), 0), lane((8, 512))
    place = (row % 4 == column // 128) & (row // 4 == column % 4 // 2)
    place = jnp.where(place, 1.0, 0.0).astype(BF16)
    hi, lo = split(total.T)
    u = dot(hi, place) + dot(lo, place)
    first_ky = lane((32, 128)) < 64
    return [
        [jnp.where(first_ky, u[32 * part:32 * part + 32, 128 * j:128 * j + 128],
                   u[64 + 32 * part:96 + 32 * part, 128 * j:128 * j + 128]) for part in range(2)]
        for j in range(4)
    ]


def inverse_x(weights, modes, inv_x):
    real, imag = 0.0, 0.0
    for j in range(4):
        wr, wi = weights(0, j), weights(1, j)
        mr, mi = modes[j]
        real += wr * mr - wi * mi
        imag += wr * mi + wi * mr
    even = lane((32, 128)) % 2 == 0
    top, bottom = jnp.where(even, real, imag), jnp.where(even, -imag, real)
    hi, lo = split(jnp.concatenate([top, bottom], 0))
    return dot(inv_x, jnp.concatenate([hi, lo, hi], 0))


def turned(arrived, roll):
    even = lax.broadcasted_iota(jnp.int32, arrived.shape, 1) % 2 == 0
    other = jnp.where(even, roll(arrived, 127, 1), -roll(arrived, 1, 1))
    return [jnp.concatenate([t[:64], t[64:]], 1) for t in (arrived.T, other.T)]


def swapped(plain):
    even = lax.broadcasted_iota(jnp.int32, plain.shape, 0) % 2 == 0
    rows = plain.shape[0]
    return jnp.where(even, pltpu.roll(plain, rows - 1, 0), -pltpu.roll(plain, 1, 0))


def inverse_y(plain, other, phases, ey_hi, ey_lo):
    his, los = [], []
    for tc, ts in phases:
        hi, lo = split(jnp.concatenate([plain * tc - other * ts, other * tc + plain * ts], 1))
        his.append(hi)
        los.append(lo)
    hi, lo = jnp.concatenate(his, 0), jnp.concatenate(los, 0)
    return dot(hi, ey_hi) + dot(lo, ey_hi) + dot(hi, ey_lo)


def inverse_z(block, inv_z):
    hi, lo = split(block.T)
    return dot(jnp.concatenate([hi, lo, hi], 1), inv_z)


def activate(value):
    cubic = value * (0.7978845608028654 + 0.035677408136300125 * (value * value))
    half = 0.5 * value
    return half + half * jnp.tanh(cubic)


def ring(step, length):
    return min(step, length - step)


ROW_STEPS = sorted(
    ((a, b) for a in range(8) for b in range(2) if a or b), key=lambda s: (-ring(s[0], 8), s))
COL_STEPS = sorted(
    ((a, b) for a in range(4) for b in range(4) if a or b),
    key=lambda s: (-ring(s[0], 4) - ring(s[1], 4), s))
PIECES = ((16, 8),)
MEETS = ((0, 8, 8, (4, 4)), (24, 28, 4, (2, 2)))


def layer_kernel(*refs):
    hbm, refs = refs[:17], refs[17:]
    out_ref, refs = refs[0], refs[1:]
    here, refs = refs[:17], refs[17:]
    (step_ref, v_ref, t_ref, fz_ref, by_ref, twy_ref, bx_ref, twx_ref, lift_ref, bias_ref, lw_ref,
     lb_ref, w_ref, ix_ref, ey_ref, twi_ref, iz_ref) = here
    (adv_ref, local_ref, s1, r1, s2, r2, s3, r3, s4, met, s5, g_ref, rows_ref, wl_ref,
     load_sem, send1, recv1, send2, recv2, send3, recv3, send4, recv4, send_m, recv_m, send5,
     recv5) = refs
    r = lax.axis_index("row")
    c = lax.axis_index("col")
    cy, cx = c // 4, c % 4
    row_peers = [((r // 2 + a) % 8) * 2 + (r + b) % 2 for a, b in ROW_STEPS]
    col_peers = [((c // 4 + a) % 4) * 4 + (c + b) % 4 for a, b in COL_STEPS]

    loads = [
        pltpu.make_async_copy(src, dst, load_sem.at[n]) for n, (src, dst) in enumerate(zip(hbm, here))
    ]
    for load in loads[:4]:
        load.start()
    barrier = pltpu.get_barrier_semaphore()
    for peer in col_peers:
        pl.semaphore_signal(
            barrier, inc=1, device_id={"row": r, "col": peer}, device_id_type=MESH)
    for peer in row_peers:
        pl.semaphore_signal(
            barrier, inc=1, device_id={"row": peer, "col": c}, device_id_type=MESH)
    for load in loads[4:]:
        load.start()

    def to_col(src, dst, send, recv, peer):
        copy = pltpu.make_async_remote_copy(
            src_ref=src, dst_ref=dst, send_sem=send, recv_sem=recv,
            device_id={"row": r, "col": peer}, device_id_type=MESH)
        copy.start()
        return copy

    def to_row(src, dst, send, recv, peer):
        copy = pltpu.make_async_remote_copy(
            src_ref=src, dst_ref=dst, send_sem=send, recv_sem=recv,
            device_id={"row": peer, "col": c}, device_id_type=MESH)
        copy.start()
        return copy

    for load in loads[:4]:
        load.wait()
    advanced = v_ref[...] + step_ref[0] * t_ref[...]
    adv_ref[...] = advanced
    z = forward_z(advanced.reshape(384, 256), fz_ref[...])
    s1[pl.ds(3, 64, stride=4), :] = jnp.zeros((64, 128), F32)
    for j in range(3):
        s1[pl.ds(j, 64, stride=4), :] = z[:, 128 * j:128 * j + 128]
    pl.semaphore_wait(barrier, 2 * (N - 1))
    first = [
        to_col(s1.at[pl.ds(pl.multiple_of(16 * peer, 16), 16)], r1.at[c], send1.at[k], recv1.at[k],
               peer)
        for k, peer in enumerate(col_peers)
    ]
    r1[c] = s1[pl.ds(pl.multiple_of(16 * c, 16), 16), :]
    for load in loads[4:]:
        load.wait()
    bx_hi, bx_lo = x_table(
        bx_ref[0], bx_ref[1], twx_ref[0, pl.ds(r, 1), :], twx_ref[1, pl.ds(r, 1), :])
    for k in (0, 4):
        rows_ref[k:k + 3] = lift_ref[...]
        rows_ref[k + 3:k + 4] = bias_ref[...]
    local_ref[...] = local_table(rows_ref[...], lw_ref[...], lb_ref[...])
    lifts = lift_tables(rows_ref[...])
    for half in range(2):
        blocks = [[[w_ref[part, ky, kz, :, 512 * half:512 * half + 512] for kz in range(2)]
                   for ky in range(2)] for part in range(2)]
        for j in range(4):
            wl_ref[half, 0, j], wl_ref[half, 1, j] = lifted_weights(blocks, lifts[j])
    for copy in first:
        copy.wait_recv()

    arrived = jnp.concatenate(
        [r1[:, 8 * part:8 * part + 8, :].reshape(128, 128) for part in range(2)], 1)
    real, imag = forward_y(arrived, by_ref[0], by_ref[1], twy_ref[0], twy_ref[1])
    partial = forward_x(real, imag, bx_hi, bx_lo, pltpu.roll)
    for g in range(4):
        for k in range(4):
            s2[4 * g + k] = partial[8 * g:8 * g + 8, 128 * k:128 * k + 128]
    second = [
        to_row(s2.at[peer], r2.at[r], send2.at[k], recv2.at[k], peer)
        for k, peer in enumerate(row_peers)
    ]
    r2[r] = s2[r]
    for copy in second:
        copy.wait_recv()
    total = jnp.sum(r2[...], axis=0)

    origin = jnp.where((r == 0) & (c == 0), 1.0, 0.0).astype(F32)
    modes = spread_modes(total, origin)
    third = []
    for half in range(2):
        s3[half] = inverse_x(
            lambda part, j: wl_ref[half, part, j], modes, ix_ref[...]).reshape(16, 8, 128)
        third.append([
            to_row(s3.at[half, peer], r3.at[half, r], send3.at[half, k], recv3.at[half, k], peer)
            for k, peer in enumerate(row_peers)
        ])
        r3[half, r] = s3[half, r]

    def arrived_half(half):
        for copy in third[half]:
            copy.wait_recv()
        return turned(r3[half].reshape(128, 128), pltpu.roll)

    def phase(k):
        return twi_ref[0, pl.ds(k, 1), :], twi_ref[1, pl.ds(k, 1), :]

    def meet(entry, plain):
        copies = []
        for axis in range(2):
            start, count = MEETS[entry][axis], MEETS[entry][2]
            first_row = 4 * (start % 16)
            place = met.at[axis, cx if axis == 0 else cy, pl.ds(32 * entry, 4 * count)]
            place[...] = plain[first_row:first_row + 4 * count]
            for d in (2, 1, 3):
                peer = 4 * cy + (cx + d) % 4 if axis == 0 else 4 * ((cy + d) % 4) + cx
                copies.append(to_col(
                    place, place, send_m.at[entry, axis, d], recv_m.at[entry, axis, d], peer))
        return copies

    plain, _ = arrived_half(0)
    meets = [meet(0, plain)]
    plain, other = arrived_half(1)
    meets.append(meet(1, plain))
    fourth = []
    for piece, (start, count) in enumerate(PIECES):
        rows = 4 * count
        near = slice(4 * (start - 16), 4 * (start - 16) + rows)
        h = inverse_y(plain[near], other[near], [phase(2 * m) for m in range(8)],
                      ey_ref[0], ey_ref[1])
        for dest in range(N):
            m, b = dest // 2, dest % 2
            s4[dest, near, :] = h[rows * m:rows * m + rows, 128 * b:128 * b + 128]
        span = pl.ds(4 * start, rows)
        fourth.append([
            to_col(s4.at[peer, pl.ds(near.start, rows)], g_ref.at[cy, cx, span],
                   send4.at[piece, k], recv4.at[piece, k], peer)
            for k, peer in enumerate(col_peers)
        ])
        g_ref[cy, cx, span, :] = s4[c, near, :]

    fifth = []
    for entry, (start_x, start_y, _, parts) in enumerate(MEETS):
        for copy in meets[entry]:
            copy.wait_recv()
        done = 0
        for count in parts:
            part = len(fifth)
            rows = 4 * count
            copies = []
            for axis, start in enumerate((start_x, start_y)):
                far = pl.ds(32 * entry + 4 * done, rows)
                plain = met[axis, :, far, :].reshape(4 * rows, 256)
                phases = [
                    phase(8 * m + cx) if axis == 0 else phase(4 * cy + 2 * m) for m in range(2)]
                table = 2 if axis == 0 else 0
                h = inverse_y(plain, swapped(plain), phases, ey_ref[table], ey_ref[table + 1])
                for t in range(4):
                    m, b = t // 2, t % 2
                    s5[part, axis, t, :, :rows] = h[
                        4 * rows * m:4 * rows * m + 4 * rows, 128 * b:128 * b + 128
                    ].reshape(4, rows, 128)
                span = pl.ds(4 * (start + done), rows)
                for d in (2, 1, 3):
                    sems = send5.at[part, axis, d], recv5.at[part, axis, d]
                    if axis == 0:
                        t = (cy + d) % 4
                        copies.append(
                            to_col(s5.at[part, 0, t, :, pl.ds(0, rows)], g_ref.at[cy, :, span], *sems, 4 * t + cx))
                    else:
                        t = (cx + d) % 4
                        copies.append(
                            to_col(s5.at[part, 1, t, :, pl.ds(0, rows)], g_ref.at[:, cx, span], *sems, 4 * cy + t))
                if axis == 0:
                    g_ref[cy, :, span, :] = s5[part, 0, cy, :, :rows]
                else:
                    g_ref[:, cx, span, :] = s5[part, 1, cx, :, :rows]
            fifth.append((copies, start_x + done, start_y + done, count))
            done += count

    def cells(start, count):
        for o in range(start, start + count, 2):
            values = inverse_z(g_ref[:, :, 4 * o:4 * o + 8, :].reshape(128, 128), iz_ref[...])
            for k in range(2):
                scale = [
                    jnp.concatenate([local_ref[o + k:o + k + 1, 128 * j:128 * j + 128]] * 2, 1)
                    for j in range(4)
                ]
                for x in range(8):
                    cell = slice(16 * x, 16 * x + 16)
                    value = values[cell, 256 * k:256 * k + 256] + scale[3]
                    for j in range(3):
                        value += scale[j] * adv_ref[j, cell, :]
                    out_ref[o + k, x] = activate(value).astype(BF16)

    for piece, (start, count) in enumerate(PIECES):
        for copy in fourth[piece]:
            copy.wait_recv()
        cells(start, count)
    for copies, start_x, start_y, count in fifth:
        for copy in copies:
            copy.wait_recv()
        cells(start_x, count)
        cells(start_y, count)
    for copies in [first, second] + third + meets + fourth + [entry[0] for entry in fifth]:
        for copy in copies:
            copy.wait_send()


def per_device(
    velocity, tendency, step_size, lift_weight, lift_bias, spectral_weight, local_weight, local_bias
):
    const = {name: jnp.asarray(a) for name, a in tables().items()}
    far = [
        step_size, velocity.reshape(3, 128, 256), tendency.reshape(3, 128, 256), const["fwd_z"],
        const["by"], const["tw_y"], const["bx"], const["tw_x"], lift_weight.T, lift_bias[None, :],
        local_weight, local_bias[None, :], spectral_weight, const["inv_x"],
        const["ey"], const["tw_i"], const["inv_z"],
    ]
    dma = pltpu.SemaphoreType.DMA
    out = pl.pallas_call(
        layer_kernel,
        out_shape=pltpu.VMEM((32, 8, 16, 256), BF16),
        in_specs=[pl.BlockSpec(memory_space=pl.ANY)] * len(far),
        out_specs=pl.BlockSpec(memory_space=pltpu.VMEM),
        scratch_shapes=[pltpu.SMEM((1,), F32)] + [pltpu.VMEM(a.shape, a.dtype) for a in far[1:]] + [
            pltpu.VMEM((3, 128, 256), F32), pltpu.VMEM((32, 512), F32),
            pltpu.VMEM((256, 128), F32), pltpu.VMEM((16, 16, 128), F32),
            pltpu.VMEM((16, 8, 128), F32), pltpu.VMEM((16, 8, 128), F32),
            pltpu.VMEM((2, 16, 8, 128), F32), pltpu.VMEM((2, 16, 8, 128), F32),
            pltpu.VMEM((16, 64, 128), F32), pltpu.VMEM((2, 4, 64, 256), F32),
            pltpu.VMEM((4, 2, 4, 4, 16, 128), F32), pltpu.VMEM((4, 4, 128, 128), F32),
            pltpu.VMEM((8, 32), F32), pltpu.VMEM((2, 2, 4, 32, 128), F32),
            dma((len(far),)), dma((N,)), dma((N,)), dma((N,)), dma((N,)),
            dma((2, N)), dma((2, N)), dma((len(PIECES), N)), dma((len(PIECES), N)),
            dma((2, 2, 4)), dma((2, 2, 4)), dma((4, 2, 4)), dma((4, 2, 4)),
        ],
        compiler_params=pltpu.CompilerParams(
            collective_id=0, has_side_effects=True, vmem_limit_bytes=VMEM_LIMIT),
        name="layer",
    )(*far)
    return out.reshape(1, 32, 8, 16, 256)


def solution(mesh):
    in_specs = (
        P(None, None, "row", "col", None),
        P(None, None, "row", "col", None),
        P(),
        P(),
        P(),
        P(None, "row", "col", None, None),
        P(),
        P(),
    )
    out_specs = P(None, None, "row", "col", None)
    return jax.shard_map(
        per_device, mesh=mesh, in_specs=in_specs, out_specs=out_specs, check_vma=False
    )
```

```python
import functools
import math

import jax
import jax.numpy as jnp
import numpy as np
from jax import lax
from jax.experimental import pallas as pl
from jax.experimental.pallas import tpu as pltpu
from jax.sharding import PartitionSpec as P

F32 = jnp.float32
BF16 = jnp.bfloat16
MESH = pl.DeviceIdType.MESH
VMEM_LIMIT = 60 * 1024 * 1024
N = 16


def split(x):
    hi = x.astype(BF16)
    lo = (x - hi.astype(F32)).astype(BF16)
    return hi, lo


def dot(a, b):
    return jnp.dot(a, b, preferred_element_type=F32)


def dot_nt(a, b):
    return lax.dot_general(a, b, (((1,), (1,)), ((), ())), preferred_element_type=F32)


def dot_exact(a, b):
    return jnp.dot(a, b, precision=lax.Precision.HIGHEST, preferred_element_type=F32)


def np_split(x):
    x = np.asarray(x, np.float64)
    hi = x.astype(np.float32).astype(jnp.bfloat16)
    lo = (x - hi.astype(np.float64)).astype(np.float32).astype(jnp.bfloat16)
    return hi, lo


@functools.lru_cache(None)
def tables():
    turn = 2.0 * np.pi
    ix = np.arange
    waves = np.where(ix(32) < 16, ix(32), ix(32) - 32)
    eye8 = np.eye(8)
    z_angle = turn * (ix(32)[:, None] * ix(256)[None, :] % 256) / 256
    z_hi, z_lo = np_split(np.concatenate([np.cos(z_angle), -np.sin(z_angle)], 0))
    fwd_z = np.concatenate([z_hi, z_lo, z_hi], 1)
    fwd_z = fwd_z.reshape(2, 16, 2, 768).transpose(2, 1, 0, 3).reshape(64, 768)
    a = turn * waves[None, :] * ix(16)[:, None] / 256
    by = np.zeros((2, 8, 16, 2, 32, 8))
    for x in range(8):
        by[0, x, :, 0, :, x] = np.cos(a)
        by[1, x, :, 0, :, x] = np.sin(a)
        by[0, x, :, 1, :, x] = -np.sin(a)
        by[1, x, :, 1, :, x] = np.cos(a)
    by_hi, by_lo = np_split(by.reshape(256, 512))
    b = turn * (waves[None, :] * ix(16)[:, None] % 16) / 16
    b = np.repeat(b, 8, axis=1)
    tw_y = np.stack([np.cos(b), np.sin(b)], 0).astype(np.float32)
    c = turn * waves[None, :] * ix(8)[:, None] / 128
    bx = []
    for quarter in (0.0, np.pi / 2):
        t = np.zeros((2, 8, 8, 8, 2, 32))
        for e in range(8):
            t[0, e, :, e, 0, :] = np.cos(c + quarter)
            t[1, e, :, e, 0, :] = np.sin(c + quarter)
            t[0, e, :, e, 1, :] = -np.sin(c + quarter)
            t[1, e, :, e, 1, :] = np.cos(c + quarter)
        bx.append(t.reshape(128, 512))
    bx = np.stack(bx, 0).astype(np.float32)
    d = turn * (waves[None, :] * ix(16)[:, None] % 16) / 16
    d = np.tile(d, (1, 16))
    tw_x = np.stack([np.cos(d), np.sin(d)], 0).astype(np.float32)
    f = turn * (waves[None, :] * ix(128)[:, None] % 128) / 128
    ex_hi, ex_lo = np_split(np.concatenate([np.cos(f), np.sin(f)], 1))
    inv_x = np.concatenate([ex_hi, ex_hi, ex_lo], 1)
    ey = []
    for apart in (1, 4):
        points = (apart * 16 * ix(2)[:, None] + ix(16)[None, :]).reshape(32)
        g = turn * (waves[:, None] * points[None, :] % 256) / 256
        t = np.zeros((2, 32, 8, 2, 8, 16))
        for x in range(8):
            for blk in range(2):
                t[0, :, x, blk, x, :] = np.cos(g[:, blk * 16:blk * 16 + 16])
                t[1, :, x, blk, x, :] = -np.sin(g[:, blk * 16:blk * 16 + 16])
        t = t.reshape(2, 16, 2, 8, 256).transpose(0, 2, 1, 3, 4)
        ey.extend(np_split(t.reshape(512, 256)))
    h = turn * (waves[None, :] * ix(16)[:, None] % 16) / 16
    h = np.repeat(h.reshape(16, 16, 2).transpose(0, 2, 1).reshape(16, 32), 8, axis=1)
    tw_i = np.stack([np.cos(h), np.sin(h)], 0).astype(np.float32)
    ez = np.zeros((16, 2, 2, 2, 2, 256))
    weight = np.where(ix(32) == 0, 1.0, 2.0)[:, None]
    cz = (weight * np.cos(z_angle)).reshape(16, 2, 256)
    sz = (-weight * np.sin(z_angle)).reshape(16, 2, 256)
    for o in range(2):
        ez[:, o, :, 0, o, :] = cz
        ez[:, o, :, 1, o, :] = sz
    ez_hi, ez_lo = np_split(ez.reshape(128, 512))
    inv_z = np.concatenate([ez_hi, ez_hi, ez_lo], 0)
    return dict(
        fwd_z=fwd_z, by=np.stack([by_hi, by_lo], 0), tw_y=tw_y, bx=bx, tw_x=tw_x,
        inv_x=inv_x, ey=np.stack(ey, 0), tw_i=tw_i, inv_z=inv_z,
    )


def forward_z(advanced, fwd_z):
    hi, lo = split(advanced)
    return dot_nt(fwd_z, jnp.concatenate([hi, hi, lo], 1))


def forward_y(arrived, by_hi, by_lo, tw_c, tw_s):
    hi, lo = split(arrived)
    u = dot(jnp.concatenate([hi, lo], 0), by_hi)
    u = u[:128] + u[128:] + dot(hi, by_lo)
    real, imag = jnp.zeros((8, 256), F32), jnp.zeros((8, 256), F32)
    for c in range(N):
        ur, ui = u[8 * c:8 * c + 8, :256], u[8 * c:8 * c + 8, 256:]
        tc, ts = tw_c[c:c + 1, :], tw_s[c:c + 1, :]
        real += ur * tc + ui * ts
        imag += ui * tc - ur * ts
    return real, imag


def x_table(bx0, bx1, tc, ts):
    return split(bx0 * tc + bx1 * ts)


def forward_x(real, imag, bx_hi, bx_lo, roll):
    low = lax.broadcasted_iota(jnp.int32, (8, 128), 1) < 64
    rows = []
    for v in range(2):
        re, im = real[:, 128 * v:128 * v + 128], imag[:, 128 * v:128 * v + 128]
        rows.append(jnp.where(low, re, roll(im, 64, 1)))
        rows.append(jnp.where(low, roll(re, 64, 1), im))
    hi, lo = split(jnp.concatenate(rows, 0))
    u = dot(jnp.concatenate([hi, lo], 0), bx_hi)
    return u[:32] + u[32:] + dot(hi, bx_lo)


def dot_nt_exact(a, b):
    return lax.dot_general(
        a, b, (((1,), (1,)), ((), ())), precision=lax.Precision.HIGHEST, preferred_element_type=F32)


def spread(rows):
    return jnp.concatenate([jnp.broadcast_to(rows[j:j + 1], (128, 32)) for j in range(4)], 0)


def identity():
    return jnp.where(
        lax.broadcasted_iota(jnp.int32, (32, 32), 0) == lax.broadcasted_iota(
            jnp.int32, (32, 32), 1), 1.0, 0.0).astype(F32)


def local_table(rows, local_weight, local_bias):
    scale = dot_nt_exact(local_weight, spread(rows))
    bias = dot_nt_exact(identity(), jnp.broadcast_to(local_bias, (128, 32)))
    return jnp.concatenate([scale[:, :384], scale[:, 384:] + bias], 1)


def lane(shape):
    return lax.broadcasted_iota(jnp.int32, shape, len(shape) - 1)


def lift_tables(rows):
    columns = dot_nt_exact(identity(), spread(rows))
    own = lax.broadcasted_iota(jnp.int32, (512, 128), 0) // 32 == lane((512, 128)) // 4 % 16
    return [
        split(jnp.where(own, jnp.concatenate([columns[:, 128 * j:128 * j + 128]] * 16, 0), 0.0))
        for j in range(4)
    ]


def lifted_weights(blocks, lift):
    stacked = jnp.concatenate([b for part in blocks for row in part for b in row], 0)
    u = dot(stacked, lift[0]) + dot(stacked, lift[1])
    first_kz, first_ky = lane((32, 128)) % 4 < 2, lane((32, 128)) < 64
    out = []
    for part in range(2):
        b = [u[128 * part + 32 * n:128 * part + 32 * n + 32] for n in range(4)]
        out.append(jnp.where(
            first_ky, jnp.where(first_kz, b[0], b[1]), jnp.where(first_kz, b[2], b[3])))
    return out


def spread_modes(total, first):
    row, column = lax.broadcasted_iota(jnp.int32, (8, 128), 0), lane((8, 128))
    total = jnp.where(row < 6, total * (1.0 / 8388608.0), 0.0)
    total = total + jnp.where((row == 6) & (column == 0), first, 0.0)
    row, column = lax.broadcasted_iota(jnp.int32, (8, 512), 0), lane((8, 512))
    j, kz = column // 128, column % 4 // 2
    place = ((row < 6) & (row == 3 * kz + j) & (j < 3)) | ((row == 6) & (j == 3) & (kz == 0))
    place = jnp.where(place, 1.0, 0.0).astype(BF16)
    hi, lo = split(total.T)
    u = dot(hi, place) + dot(lo, place)
    first_ky = lane((32, 128)) < 64
    return [
        [jnp.where(first_ky, u[32 * part:32 * part + 32, 128 * j:128 * j + 128],
                   u[64 + 32 * part:96 + 32 * part, 128 * j:128 * j + 128]) for part in range(2)]
        for j in range(4)
    ]


def inverse_x(weights, modes, inv_x):
    real, imag = 0.0, 0.0
    for j in range(4):
        wr, wi = weights(0, j), weights(1, j)
        mr, mi = modes[j]
        real += wr * mr - wi * mi
        imag += wr * mi + wi * mr
    even = lane((32, 128)) % 2 == 0
    top, bottom = jnp.where(even, real, imag), jnp.where(even, -imag, real)
    hi, lo = split(jnp.concatenate([top, bottom], 0))
    return dot(inv_x, jnp.concatenate([hi, lo, hi], 0))


def turned(arrived, roll):
    even = lax.broadcasted_iota(jnp.int32, arrived.shape, 1) % 2 == 0
    other = jnp.where(even, roll(arrived, 127, 1), -roll(arrived, 1, 1))
    return [jnp.concatenate([t[:64], t[64:]], 1) for t in (arrived.T, other.T)]


def swapped(plain):
    even = lax.broadcasted_iota(jnp.int32, plain.shape, 0) % 2 == 0
    rows = plain.shape[0]
    return jnp.where(even, pltpu.roll(plain, rows - 1, 0), -pltpu.roll(plain, 1, 0))


def inverse_y(plain, other, phases, ey_hi, ey_lo):
    his, los = [], []
    for tc, ts in phases:
        hi, lo = split(jnp.concatenate([plain * tc - other * ts, other * tc + plain * ts], 1))
        his.append(hi)
        los.append(lo)
    hi, lo = jnp.concatenate(his, 0), jnp.concatenate(los, 0)
    return dot(hi, ey_hi) + dot(lo, ey_hi) + dot(hi, ey_lo)


def inverse_z(block, inv_z):
    hi, lo = split(block.T)
    return dot(jnp.concatenate([hi, lo, hi], 1), inv_z)


def activate(value):
    cubic = value * (0.7978845608028654 + 0.035677408136300125 * (value * value))
    half = 0.5 * value
    return half + half * jnp.tanh(cubic)


def ring(step, length):
    return min(step, length - step)


ROW_STEPS = sorted(
    ((a, b) for a in range(8) for b in range(2) if a or b), key=lambda s: (-ring(s[0], 8), s))
COL_STEPS = sorted(
    ((a, b) for a in range(4) for b in range(4) if a or b),
    key=lambda s: (-ring(s[0], 4) - ring(s[1], 4), s))
PIECES = ((16, 8),)
MEETS = ((0, 8, 8, (4, 4)), (24, 28, 4, (2, 2)))


def layer_kernel(*refs):
    hbm, refs = refs[:17], refs[17:]
    out_ref, refs = refs[0], refs[1:]
    here, refs = refs[:17], refs[17:]
    (step_ref, v_ref, t_ref, fz_ref, by_ref, twy_ref, bx_ref, twx_ref, lift_ref, bias_ref, lw_ref,
     lb_ref, w_ref, ix_ref, ey_ref, twi_ref, iz_ref) = here
    (adv_ref, local_ref, s1, r1, s2, r2, s3, r3, s4, met, s5, g_ref, rows_ref, wl_ref,
     load_sem, send1, recv1, send2, recv2, send3, recv3, send4, recv4, send_m, recv_m, send5,
     recv5) = refs
    r = lax.axis_index("row")
    c = lax.axis_index("col")
    cy, cx = c // 4, c % 4
    row_peers = [((r // 2 + a) % 8) * 2 + (r + b) % 2 for a, b in ROW_STEPS]
    col_peers = [((c // 4 + a) % 4) * 4 + (c + b) % 4 for a, b in COL_STEPS]

    loads = [
        pltpu.make_async_copy(src, dst, load_sem.at[n]) for n, (src, dst) in enumerate(zip(hbm, here))
    ]
    for load in loads[:4]:
        load.start()
    barrier = pltpu.get_barrier_semaphore()
    for peer in col_peers:
        pl.semaphore_signal(
            barrier, inc=1, device_id={"row": r, "col": peer}, device_id_type=MESH)
    for peer in row_peers:
        pl.semaphore_signal(
            barrier, inc=1, device_id={"row": peer, "col": c}, device_id_type=MESH)
    for load in loads[4:]:
        load.start()

    def to_col(src, dst, send, recv, peer):
        copy = pltpu.make_async_remote_copy(
            src_ref=src, dst_ref=dst, send_sem=send, recv_sem=recv,
            device_id={"row": r, "col": peer}, device_id_type=MESH)
        copy.start()
        return copy

    def to_row(src, dst, send, recv, peer):
        copy = pltpu.make_async_remote_copy(
            src_ref=src, dst_ref=dst, send_sem=send, recv_sem=recv,
            device_id={"row": peer, "col": c}, device_id_type=MESH)
        copy.start()
        return copy

    for load in loads[:4]:
        load.wait()
    advanced = v_ref[...] + step_ref[0] * t_ref[...]
    adv_ref[...] = advanced
    z = forward_z(advanced.reshape(384, 256), fz_ref[...])
    for kz in range(2):
        for j in range(3):
            s1[pl.ds(3 * kz + j, 32, stride=8), :] = z[32 * kz:32 * kz + 32, 128 * j:128 * j + 128]
    pl.semaphore_wait(barrier, 2 * (N - 1))
    used = pl.ds(0, 6)
    first = [
        to_col(s1.reshape(16, 2, 8, 128).at[peer, :, used], r1.at[c, :, used], send1.at[k],
               recv1.at[k], peer)
        for k, peer in enumerate(col_peers)
    ]
    r1[c] = s1[pl.ds(pl.multiple_of(16 * c, 16), 16), :].reshape(2, 8, 128)
    for load in loads[4:]:
        load.wait()
    bx_hi, bx_lo = x_table(
        bx_ref[0], bx_ref[1], twx_ref[0, pl.ds(r, 1), :], twx_ref[1, pl.ds(r, 1), :])
    for k in (0, 4):
        rows_ref[k:k + 3] = lift_ref[...]
        rows_ref[k + 3:k + 4] = bias_ref[...]
    local_ref[...] = local_table(rows_ref[...], lw_ref[...], lb_ref[...])
    lifts = lift_tables(rows_ref[...])
    for half in range(2):
        blocks = [[[w_ref[part, ky, kz, :, 512 * half:512 * half + 512] for kz in range(2)]
                   for ky in range(2)] for part in range(2)]
        for j in range(4):
            wl_ref[half, 0, j], wl_ref[half, 1, j] = lifted_weights(blocks, lifts[j])
    for copy in first:
        copy.wait_recv()

    arrived = jnp.concatenate(
        [r1[:, part].reshape(128, 128) for part in range(2)], 1)
    real, imag = forward_y(arrived, by_ref[0], by_ref[1], twy_ref[0], twy_ref[1])
    partial = forward_x(real, imag, bx_hi, bx_lo, pltpu.roll)
    for g in range(4):
        for k in range(4):
            s2[4 * g + k] = partial[8 * g:8 * g + 8, 128 * k:128 * k + 128]
    second = [
        to_row(s2.at[peer, used], r2.at[r, used], send2.at[k], recv2.at[k], peer)
        for k, peer in enumerate(row_peers)
    ]
    r2[r] = s2[r]
    for copy in second:
        copy.wait_recv()
    total = jnp.sum(r2[...], axis=0)

    origin = jnp.where((r == 0) & (c == 0), 1.0, 0.0).astype(F32)
    modes = spread_modes(total, origin)
    third = []
    for half in range(2):
        s3[half] = inverse_x(
            lambda part, j: wl_ref[half, part, j], modes, ix_ref[...]).reshape(16, 8, 128)
        third.append([
            to_row(s3.at[half, peer], r3.at[half, r], send3.at[half, k], recv3.at[half, k], peer)
            for k, peer in enumerate(row_peers)
        ])
        r3[half, r] = s3[half, r]

    def arrived_half(half):
        for copy in third[half]:
            copy.wait_recv()
        return turned(r3[half].reshape(128, 128), pltpu.roll)

    def phase(k):
        return twi_ref[0, pl.ds(k, 1), :], twi_ref[1, pl.ds(k, 1), :]

    def meet(entry, plain):
        copies = []
        for axis in range(2):
            start, count = MEETS[entry][axis], MEETS[entry][2]
            first_row = 4 * (start % 16)
            place = met.at[axis, cx if axis == 0 else cy, pl.ds(32 * entry, 4 * count)]
            place[...] = plain[first_row:first_row + 4 * count]
            for d in (2, 1, 3):
                peer = 4 * cy + (cx + d) % 4 if axis == 0 else 4 * ((cy + d) % 4) + cx
                copies.append(to_col(
                    place, place, send_m.at[entry, axis, d], recv_m.at[entry, axis, d], peer))
        return copies

    plain, _ = arrived_half(0)
    meets = [meet(0, plain)]
    plain, other = arrived_half(1)
    meets.append(meet(1, plain))
    fourth = []
    for piece, (start, count) in enumerate(PIECES):
        rows = 4 * count
        near = slice(4 * (start - 16), 4 * (start - 16) + rows)
        h = inverse_y(plain[near], other[near], [phase(2 * m) for m in range(8)],
                      ey_ref[0], ey_ref[1])
        for dest in range(N):
            m, b = dest // 2, dest % 2
            s4[dest, near, :] = h[rows * m:rows * m + rows, 128 * b:128 * b + 128]
        span = pl.ds(4 * start, rows)
        fourth.append([
            to_col(s4.at[peer, pl.ds(near.start, rows)], g_ref.at[cy, cx, span],
                   send4.at[piece, k], recv4.at[piece, k], peer)
            for k, peer in enumerate(col_peers)
        ])
        g_ref[cy, cx, span, :] = s4[c, near, :]

    fifth = []
    for entry, (start_x, start_y, _, parts) in enumerate(MEETS):
        for copy in meets[entry]:
            copy.wait_recv()
        done = 0
        for count in parts:
            part = len(fifth)
            rows = 4 * count
            copies = []
            for axis, start in enumerate((start_x, start_y)):
                far = pl.ds(32 * entry + 4 * done, rows)
                plain = met[axis, :, far, :].reshape(4 * rows, 256)
                phases = [
                    phase(8 * m + cx) if axis == 0 else phase(4 * cy + 2 * m) for m in range(2)]
                table = 2 if axis == 0 else 0
                h = inverse_y(plain, swapped(plain), phases, ey_ref[table], ey_ref[table + 1])
                for t in range(4):
                    m, b = t // 2, t % 2
                    s5[part, axis, t, :, :rows] = h[
                        4 * rows * m:4 * rows * m + 4 * rows, 128 * b:128 * b + 128
                    ].reshape(4, rows, 128)
                span = pl.ds(4 * (start + done), rows)
                for d in (2, 1, 3):
                    sems = send5.at[part, axis, d], recv5.at[part, axis, d]
                    if axis == 0:
                        t = (cy + d) % 4
                        copies.append(
                            to_col(s5.at[part, 0, t, :, pl.ds(0, rows)], g_ref.at[cy, :, span], *sems, 4 * t + cx))
                    else:
                        t = (cx + d) % 4
                        copies.append(
                            to_col(s5.at[part, 1, t, :, pl.ds(0, rows)], g_ref.at[:, cx, span], *sems, 4 * cy + t))
                if axis == 0:
                    g_ref[cy, :, span, :] = s5[part, 0, cy, :, :rows]
                else:
                    g_ref[:, cx, span, :] = s5[part, 1, cx, :, :rows]
            fifth.append((copies, start_x + done, start_y + done, count))
            done += count

    def cells(start, count):
        for o in range(start, start + count, 2):
            values = inverse_z(g_ref[:, :, 4 * o:4 * o + 8, :].reshape(128, 128), iz_ref[...])
            for k in range(2):
                scale = [
                    jnp.concatenate([local_ref[o + k:o + k + 1, 128 * j:128 * j + 128]] * 2, 1)
                    for j in range(4)
                ]
                for x in range(8):
                    cell = slice(16 * x, 16 * x + 16)
                    value = values[cell, 256 * k:256 * k + 256] + scale[3]
                    for j in range(3):
                        value += scale[j] * adv_ref[j, cell, :]
                    out_ref[o + k, x] = activate(value).astype(BF16)

    for piece, (start, count) in enumerate(PIECES):
        for copy in fourth[piece]:
            copy.wait_recv()
        cells(start, count)
    for copies in [first, second] + third + meets + fourth:
        for copy in copies:
            copy.wait_send()
    for part, (copies, start_x, start_y, count) in enumerate(fifth):
        if part:
            for copy in fifth[part - 1][0]:
                copy.wait_send()
        for copy in copies:
            copy.wait_recv()
        cells(start_x, count)
        cells(start_y, count)
    for copy in fifth[-1][0]:
        copy.wait_send()


def per_device(
    velocity, tendency, step_size, lift_weight, lift_bias, spectral_weight, local_weight, local_bias
):
    const = {name: jnp.asarray(a) for name, a in tables().items()}
    far = [
        step_size, velocity.reshape(3, 128, 256), tendency.reshape(3, 128, 256), const["fwd_z"],
        const["by"], const["tw_y"], const["bx"], const["tw_x"], lift_weight.T, lift_bias[None, :],
        local_weight, local_bias[None, :], spectral_weight, const["inv_x"],
        const["ey"], const["tw_i"], const["inv_z"],
    ]
    dma = pltpu.SemaphoreType.DMA
    out = pl.pallas_call(
        layer_kernel,
        out_shape=pltpu.VMEM((32, 8, 16, 256), BF16),
        in_specs=[pl.BlockSpec(memory_space=pl.ANY)] * len(far),
        out_specs=pl.BlockSpec(memory_space=pltpu.VMEM),
        scratch_shapes=[pltpu.SMEM((1,), F32)] + [pltpu.VMEM(a.shape, a.dtype) for a in far[1:]] + [
            pltpu.VMEM((3, 128, 256), F32), pltpu.VMEM((32, 512), F32),
            pltpu.VMEM((256, 128), F32), pltpu.VMEM((16, 2, 8, 128), F32),
            pltpu.VMEM((16, 8, 128), F32), pltpu.VMEM((16, 8, 128), F32),
            pltpu.VMEM((2, 16, 8, 128), F32), pltpu.VMEM((2, 16, 8, 128), F32),
            pltpu.VMEM((16, 64, 128), F32), pltpu.VMEM((2, 4, 64, 256), F32),
            pltpu.VMEM((4, 2, 4, 4, 16, 128), F32), pltpu.VMEM((4, 4, 128, 128), F32),
            pltpu.VMEM((8, 32), F32), pltpu.VMEM((2, 2, 4, 32, 128), F32),
            dma((len(far),)), dma((N,)), dma((N,)), dma((N,)), dma((N,)),
            dma((2, N)), dma((2, N)), dma((len(PIECES), N)), dma((len(PIECES), N)),
            dma((2, 2, 4)), dma((2, 2, 4)), dma((4, 2, 4)), dma((4, 2, 4)),
        ],
        compiler_params=pltpu.CompilerParams(
            collective_id=0, has_side_effects=True, vmem_limit_bytes=VMEM_LIMIT),
        name="layer",
    )(*far)
    return out.reshape(1, 32, 8, 16, 256)


def solution(mesh):
    in_specs = (
        P(None, None, "row", "col", None),
        P(None, None, "row", "col", None),
        P(),
        P(),
        P(),
        P(None, "row", "col", None, None),
        P(),
        P(),
    )
    out_specs = P(None, None, "row", "col", None)
    return jax.shard_map(
        per_device, mesh=mesh, in_specs=in_specs, out_specs=out_specs, check_vma=False
    )
```

```python
import functools
import math

import jax
import jax.numpy as jnp
import numpy as np
from jax import lax
from jax.experimental import pallas as pl
from jax.experimental.pallas import tpu as pltpu
from jax.sharding import PartitionSpec as P

F32 = jnp.float32
BF16 = jnp.bfloat16
MESH = pl.DeviceIdType.MESH
VMEM_LIMIT = 60 * 1024 * 1024
N = 16


def split(x):
    hi = x.astype(BF16)
    lo = (x - hi.astype(F32)).astype(BF16)
    return hi, lo


def dot(a, b):
    return jnp.dot(a, b, preferred_element_type=F32)


def dot_nt(a, b):
    return lax.dot_general(a, b, (((1,), (1,)), ((), ())), preferred_element_type=F32)


def dot_exact(a, b):
    return jnp.dot(a, b, precision=lax.Precision.HIGHEST, preferred_element_type=F32)


def np_split(x):
    x = np.asarray(x, np.float64)
    hi = x.astype(np.float32).astype(jnp.bfloat16)
    lo = (x - hi.astype(np.float64)).astype(np.float32).astype(jnp.bfloat16)
    return hi, lo


@functools.lru_cache(None)
def tables():
    turn = 2.0 * np.pi
    ix = np.arange
    waves = np.where(ix(32) < 16, ix(32), ix(32) - 32)
    eye8 = np.eye(8)
    z_angle = turn * (ix(32)[:, None] * ix(256)[None, :] % 256) / 256
    z_hi, z_lo = np_split(np.concatenate([np.cos(z_angle), -np.sin(z_angle)], 0))
    fwd_z = np.concatenate([z_hi, z_lo, z_hi], 1)
    fwd_z = fwd_z.reshape(2, 16, 2, 768).transpose(1, 0, 2, 3).reshape(64, 768)
    a = turn * waves[None, :] * ix(16)[:, None] / 256
    by = np.zeros((2, 8, 16, 2, 32, 8))
    for x in range(8):
        by[0, x, :, 0, :, x] = np.cos(a)
        by[1, x, :, 0, :, x] = np.sin(a)
        by[0, x, :, 1, :, x] = -np.sin(a)
        by[1, x, :, 1, :, x] = np.cos(a)
    by_hi, by_lo = np_split(by.reshape(256, 512))
    b = turn * (waves[None, :] * ix(16)[:, None] % 16) / 16
    b = np.repeat(b, 8, axis=1)
    tw_y = np.stack([np.cos(b), np.sin(b)], 0).astype(np.float32)
    c = turn * waves[None, :] * ix(8)[:, None] / 128
    bx = []
    for quarter in (0.0, np.pi / 2):
        t = np.zeros((2, 8, 8, 8, 2, 32))
        for e in range(8):
            t[0, e, :, e, 0, :] = np.cos(c + quarter)
            t[1, e, :, e, 0, :] = np.sin(c + quarter)
            t[0, e, :, e, 1, :] = -np.sin(c + quarter)
            t[1, e, :, e, 1, :] = np.cos(c + quarter)
        bx.append(t.reshape(128, 512))
    bx = np.stack(bx, 0).astype(np.float32)
    d = turn * (waves[None, :] * ix(16)[:, None] % 16) / 16
    d = np.tile(d, (1, 16))
    tw_x = np.stack([np.cos(d), np.sin(d)], 0).astype(np.float32)
    f = turn * (waves[None, :] * ix(128)[:, None] % 128) / 128
    ex_hi, ex_lo = np_split(np.concatenate([np.cos(f), np.sin(f)], 1))
    inv_x = np.concatenate([ex_hi, ex_hi, ex_lo], 1)
    ey = []
    for apart in (1, 4):
        points = (apart * 16 * ix(2)[:, None] + ix(16)[None, :]).reshape(32)
        g = turn * (waves[:, None] * points[None, :] % 256) / 256
        t = np.zeros((2, 32, 8, 2, 8, 16))
        for x in range(8):
            for blk in range(2):
                t[0, :, x, blk, x, :] = np.cos(g[:, blk * 16:blk * 16 + 16])
                t[1, :, x, blk, x, :] = -np.sin(g[:, blk * 16:blk * 16 + 16])
        t = t.reshape(2, 16, 2, 8, 256).transpose(0, 2, 1, 3, 4)
        ey.extend(np_split(t.reshape(512, 256)))
    h = turn * (waves[None, :] * ix(16)[:, None] % 16) / 16
    h = np.repeat(h.reshape(16, 16, 2).transpose(0, 2, 1).reshape(16, 32), 8, axis=1)
    tw_i = np.stack([np.cos(h), np.sin(h)], 0).astype(np.float32)
    ez = np.zeros((16, 2, 2, 2, 2, 256))
    weight = np.where(ix(32) == 0, 1.0, 2.0)[:, None]
    cz = (weight * np.cos(z_angle)).reshape(16, 2, 256)
    sz = (-weight * np.sin(z_angle)).reshape(16, 2, 256)
    for o in range(2):
        ez[:, o, :, 0, o, :] = cz
        ez[:, o, :, 1, o, :] = sz
    ez_hi, ez_lo = np_split(0.5 * ez.reshape(128, 512))
    inv_z = np.concatenate([ez_hi, ez_hi, ez_lo], 0)
    return dict(
        fwd_z=fwd_z, by=np.stack([by_hi, by_lo], 0), tw_y=tw_y, bx=bx, tw_x=tw_x,
        inv_x=inv_x, ey=np.stack(ey, 0), tw_i=tw_i, inv_z=inv_z,
    )


def forward_z(advanced, fwd_z):
    hi, lo = split(advanced)
    return dot_nt(fwd_z, jnp.concatenate([hi, hi, lo], 1))


def forward_y(arrived, by_hi, by_lo, tw_c, tw_s):
    hi, lo = split(arrived)
    u = dot(jnp.concatenate([hi, lo], 0), by_hi)
    u = u[:128] + u[128:] + dot(hi, by_lo)
    real, imag = jnp.zeros((8, 256), F32), jnp.zeros((8, 256), F32)
    for c in range(N):
        ur, ui = u[8 * c:8 * c + 8, :256], u[8 * c:8 * c + 8, 256:]
        tc, ts = tw_c[c:c + 1, :], tw_s[c:c + 1, :]
        real += ur * tc + ui * ts
        imag += ui * tc - ur * ts
    return real, imag


def x_table(bx0, bx1, tc, ts):
    return split(bx0 * tc + bx1 * ts)


def forward_x(real, imag, bx_hi, bx_lo, roll):
    low = lax.broadcasted_iota(jnp.int32, (8, 128), 1) < 64
    rows = []
    for v in range(2):
        re, im = real[:, 128 * v:128 * v + 128], imag[:, 128 * v:128 * v + 128]
        rows.append(jnp.where(low, re, roll(im, 64, 1)))
        rows.append(jnp.where(low, roll(re, 64, 1), im))
    hi, lo = split(jnp.concatenate(rows, 0))
    u = dot(jnp.concatenate([hi, lo], 0), bx_hi)
    return u[:32] + u[32:] + dot(hi, bx_lo)


def dot_nt_exact(a, b):
    return lax.dot_general(
        a, b, (((1,), (1,)), ((), ())), precision=lax.Precision.HIGHEST, preferred_element_type=F32)


def spread(rows):
    return jnp.concatenate([jnp.broadcast_to(rows[j:j + 1], (128, 32)) for j in range(4)], 0)


def identity():
    return jnp.where(
        lax.broadcasted_iota(jnp.int32, (32, 32), 0) == lax.broadcasted_iota(
            jnp.int32, (32, 32), 1), 1.0, 0.0).astype(F32)


def local_table(rows, local_weight, local_bias):
    scale = dot_nt_exact(local_weight, spread(rows))
    bias = dot_nt_exact(identity(), jnp.broadcast_to(local_bias, (128, 32)))
    return jnp.concatenate([scale[:, :384], scale[:, 384:] + bias], 1)


def lane(shape):
    return lax.broadcasted_iota(jnp.int32, shape, len(shape) - 1)


def lift_tables(rows):
    columns = dot_nt_exact(identity(), spread(rows))
    own = lax.broadcasted_iota(jnp.int32, (512, 128), 0) // 32 == lane((512, 128)) // 4 % 16
    return [
        split(jnp.where(own, jnp.concatenate([columns[:, 128 * j:128 * j + 128]] * 16, 0), 0.0))
        for j in range(4)
    ]


def lifted_weights(blocks, lift):
    stacked = jnp.concatenate([b for part in blocks for row in part for b in row], 0)
    u = dot(stacked, lift[0]) + dot(stacked, lift[1])
    first_kz, first_ky = lane((32, 128)) % 4 < 2, lane((32, 128)) < 64
    out = []
    for part in range(2):
        b = [u[128 * part + 32 * n:128 * part + 32 * n + 32] for n in range(4)]
        out.append(jnp.where(
            first_ky, jnp.where(first_kz, b[0], b[1]), jnp.where(first_kz, b[2], b[3])))
    return out


def spread_modes(total, first):
    row, column = lax.broadcasted_iota(jnp.int32, (8, 128), 0), lane((8, 128))
    total = total * (1.0 / 8388608.0) + jnp.where((row == 3) & (column == 0), first, 0.0)
    row, column = lax.broadcasted_iota(jnp.int32, (8, 512), 0), lane((8, 512))
    place = (row % 4 == column // 128) & (row // 4 == column % 4 // 2)
    place = jnp.where(place, 1.0, 0.0).astype(BF16)
    hi, lo = split(total.T)
    u = dot(hi, place) + dot(lo, place)
    first_ky = lane((32, 128)) < 64
    return [
        [jnp.where(first_ky, u[32 * part:32 * part + 32, 128 * j:128 * j + 128],
                   u[64 + 32 * part:96 + 32 * part, 128 * j:128 * j + 128]) for part in range(2)]
        for j in range(4)
    ]


def inverse_x(weights, modes, inv_x):
    real, imag = 0.0, 0.0
    for j in range(4):
        wr, wi = weights(0, j), weights(1, j)
        mr, mi = modes[j]
        real += wr * mr - wi * mi
        imag += wr * mi + wi * mr
    even = lane((32, 128)) % 2 == 0
    top, bottom = jnp.where(even, real, imag), jnp.where(even, -imag, real)
    hi, lo = split(jnp.concatenate([top, bottom], 0))
    return dot(inv_x, jnp.concatenate([hi, lo, hi], 0))


def turned(arrived, roll):
    even = lax.broadcasted_iota(jnp.int32, arrived.shape, 1) % 2 == 0
    other = jnp.where(even, roll(arrived, 127, 1), -roll(arrived, 1, 1))
    return [jnp.concatenate([t[:64], t[64:]], 1) for t in (arrived.T, other.T)]


def swapped(plain):
    even = lax.broadcasted_iota(jnp.int32, plain.shape, 0) % 2 == 0
    rows = plain.shape[0]
    return jnp.where(even, pltpu.roll(plain, rows - 1, 0), -pltpu.roll(plain, 1, 0))


def inverse_y(plain, other, phases, ey_hi, ey_lo):
    his, los = [], []
    for tc, ts in phases:
        hi, lo = split(jnp.concatenate([plain * tc - other * ts, other * tc + plain * ts], 1))
        his.append(hi)
        los.append(lo)
    hi, lo = jnp.concatenate(his, 0), jnp.concatenate(los, 0)
    return dot(hi, ey_hi) + dot(lo, ey_hi) + dot(hi, ey_lo)


def inverse_z(block, inv_z):
    hi, lo = split(block.T)
    return dot(jnp.concatenate([hi, lo, hi], 1), inv_z)


def activate(half):
    cubic = half * (1.5957691216057308 + 0.285419265090401 * (half * half))
    return half + half * jnp.tanh(cubic)


def ring(step, length):
    return min(step, length - step)


ROW_STEPS = sorted(
    ((a, b) for a in range(8) for b in range(2) if a or b), key=lambda s: (-ring(s[0], 8), s))
COL_STEPS = sorted(
    ((a, b) for a in range(4) for b in range(4) if a or b),
    key=lambda s: (-ring(s[0], 4) - ring(s[1], 4), s))
PIECES = ((16, 8),)
MEETS = ((0, 8, 8, (4, 4)), (24, 28, 4, (2, 2)))


def layer_kernel(*refs):
    hbm, refs = refs[:17], refs[17:]
    out_ref, refs = refs[0], refs[1:]
    here, refs = refs[:17], refs[17:]
    (step_ref, v_ref, t_ref, fz_ref, by_ref, twy_ref, bx_ref, twx_ref, lift_ref, bias_ref, lw_ref,
     lb_ref, w_ref, ix_ref, ey_ref, twi_ref, iz_ref) = here
    (adv_ref, local_ref, s1, r1, s2, r2, s3, r3, s4, met, s5, g_ref, rows_ref, wl_ref,
     load_sem, send1, recv1, send2, recv2, send3, recv3, send4, recv4, send_m, recv_m, send5,
     recv5) = refs
    r = lax.axis_index("row")
    c = lax.axis_index("col")
    cy, cx = c // 4, c % 4
    row_peers = [((r // 2 + a) % 8) * 2 + (r + b) % 2 for a, b in ROW_STEPS]
    col_peers = [((c // 4 + a) % 4) * 4 + (c + b) % 4 for a, b in COL_STEPS]

    loads = [
        pltpu.make_async_copy(src, dst, load_sem.at[n]) for n, (src, dst) in enumerate(zip(hbm, here))
    ]
    for load in loads[:4]:
        load.start()
    barrier = pltpu.get_barrier_semaphore()
    for peer in col_peers:
        pl.semaphore_signal(
            barrier, inc=1, device_id={"row": r, "col": peer}, device_id_type=MESH)
    for peer in row_peers:
        pl.semaphore_signal(
            barrier, inc=1, device_id={"row": peer, "col": c}, device_id_type=MESH)
    for load in loads[4:]:
        load.start()

    def to_col(src, dst, send, recv, peer):
        copy = pltpu.make_async_remote_copy(
            src_ref=src, dst_ref=dst, send_sem=send, recv_sem=recv,
            device_id={"row": r, "col": peer}, device_id_type=MESH)
        copy.start()
        return copy

    def to_row(src, dst, send, recv, peer):
        copy = pltpu.make_async_remote_copy(
            src_ref=src, dst_ref=dst, send_sem=send, recv_sem=recv,
            device_id={"row": peer, "col": c}, device_id_type=MESH)
        copy.start()
        return copy

    for load in loads[:4]:
        load.wait()
    advanced = v_ref[...] + step_ref[0] * t_ref[...]
    adv_ref[...] = advanced
    z = forward_z(advanced.reshape(384, 256), fz_ref[...])
    s1[pl.ds(3, 64, stride=4), :] = jnp.zeros((64, 128), F32)
    for j in range(3):
        s1[pl.ds(j, 64, stride=4), :] = z[:, 128 * j:128 * j + 128]
    pl.semaphore_wait(barrier, 2 * (N - 1))
    first = [
        to_col(s1.at[pl.ds(pl.multiple_of(16 * peer, 16), 16)], r1.at[c], send1.at[k], recv1.at[k],
               peer)
        for k, peer in enumerate(col_peers)
    ]
    r1[c] = s1[pl.ds(pl.multiple_of(16 * c, 16), 16), :]
    for load in loads[4:]:
        load.wait()
    bx_hi, bx_lo = x_table(
        bx_ref[0], bx_ref[1], twx_ref[0, pl.ds(r, 1), :], twx_ref[1, pl.ds(r, 1), :])
    for k in (0, 4):
        rows_ref[k:k + 3] = lift_ref[...]
        rows_ref[k + 3:k + 4] = bias_ref[...]
    local_ref[...] = 0.5 * local_table(rows_ref[...], lw_ref[...], lb_ref[...])
    lifts = lift_tables(rows_ref[...])
    for half in range(2):
        blocks = [[[w_ref[part, ky, kz, :, 512 * half:512 * half + 512] for kz in range(2)]
                   for ky in range(2)] for part in range(2)]
        for j in range(4):
            wl_ref[half, 0, j], wl_ref[half, 1, j] = lifted_weights(blocks, lifts[j])
    for copy in first:
        copy.wait_recv()

    arrived = jnp.concatenate(
        [r1[:, 8 * part:8 * part + 8, :].reshape(128, 128) for part in range(2)], 1)
    real, imag = forward_y(arrived, by_ref[0], by_ref[1], twy_ref[0], twy_ref[1])
    partial = forward_x(real, imag, bx_hi, bx_lo, pltpu.roll)
    for g in range(4):
        for k in range(4):
            s2[4 * g + k] = partial[8 * g:8 * g + 8, 128 * k:128 * k + 128]
    second = [
        to_row(s2.at[peer], r2.at[r], send2.at[k], recv2.at[k], peer)
        for k, peer in enumerate(row_peers)
    ]
    r2[r] = s2[r]
    for copy in second:
        copy.wait_recv()
    total = jnp.sum(r2[...], axis=0)

    origin = jnp.where((r == 0) & (c == 0), 1.0, 0.0).astype(F32)
    modes = spread_modes(total, origin)
    third = []
    for half in range(2):
        s3[half] = inverse_x(
            lambda part, j: wl_ref[half, part, j], modes, ix_ref[...]).reshape(16, 8, 128)
        third.append([
            to_row(s3.at[half, peer], r3.at[half, r], send3.at[half, k], recv3.at[half, k], peer)
            for k, peer in enumerate(row_peers)
        ])
        r3[half, r] = s3[half, r]

    def arrived_half(half):
        for copy in third[half]:
            copy.wait_recv()
        return turned(r3[half].reshape(128, 128), pltpu.roll)

    def phase(k):
        return twi_ref[0, pl.ds(k, 1), :], twi_ref[1, pl.ds(k, 1), :]

    def meet(entry, plain):
        copies = []
        for axis in range(2):
            start, count = MEETS[entry][axis], MEETS[entry][2]
            first_row = 4 * (start % 16)
            place = met.at[axis, cx if axis == 0 else cy, pl.ds(32 * entry, 4 * count)]
            place[...] = plain[first_row:first_row + 4 * count]
            for d in (2, 1, 3):
                peer = 4 * cy + (cx + d) % 4 if axis == 0 else 4 * ((cy + d) % 4) + cx
                copies.append(to_col(
                    place, place, send_m.at[entry, axis, d], recv_m.at[entry, axis, d], peer))
        return copies

    plain, _ = arrived_half(0)
    meets = [meet(0, plain)]
    plain, other = arrived_half(1)
    meets.append(meet(1, plain))
    fourth = []
    for piece, (start, count) in enumerate(PIECES):
        rows = 4 * count
        near = slice(4 * (start - 16), 4 * (start - 16) + rows)
        h = inverse_y(plain[near], other[near], [phase(2 * m) for m in range(8)],
                      ey_ref[0], ey_ref[1])
        for dest in range(N):
            m, b = dest // 2, dest % 2
            s4[dest, near, :] = h[rows * m:rows * m + rows, 128 * b:128 * b + 128]
        span = pl.ds(4 * start, rows)
        fourth.append([
            to_col(s4.at[peer, pl.ds(near.start, rows)], g_ref.at[cy, cx, span],
                   send4.at[piece, k], recv4.at[piece, k], peer)
            for k, peer in enumerate(col_peers)
        ])
        g_ref[cy, cx, span, :] = s4[c, near, :]

    fifth = []
    for entry, (start_x, start_y, _, parts) in enumerate(MEETS):
        for copy in meets[entry]:
            copy.wait_recv()
        done = 0
        for count in parts:
            part = len(fifth)
            rows = 4 * count
            copies = []
            for axis, start in enumerate((start_x, start_y)):
                far = pl.ds(32 * entry + 4 * done, rows)
                plain = met[axis, :, far, :].reshape(4 * rows, 256)
                phases = [
                    phase(8 * m + cx) if axis == 0 else phase(4 * cy + 2 * m) for m in range(2)]
                table = 2 if axis == 0 else 0
                h = inverse_y(plain, swapped(plain), phases, ey_ref[table], ey_ref[table + 1])
                for t in range(4):
                    m, b = t // 2, t % 2
                    s5[part, axis, t, :, :rows] = h[
                        4 * rows * m:4 * rows * m + 4 * rows, 128 * b:128 * b + 128
                    ].reshape(4, rows, 128)
                span = pl.ds(4 * (start + done), rows)
                for d in (2, 1, 3):
                    sems = send5.at[part, axis, d], recv5.at[part, axis, d]
                    if axis == 0:
                        t = (cy + d) % 4
                        copies.append(
                            to_col(s5.at[part, 0, t, :, pl.ds(0, rows)], g_ref.at[cy, :, span], *sems, 4 * t + cx))
                    else:
                        t = (cx + d) % 4
                        copies.append(
                            to_col(s5.at[part, 1, t, :, pl.ds(0, rows)], g_ref.at[:, cx, span], *sems, 4 * cy + t))
                if axis == 0:
                    g_ref[cy, :, span, :] = s5[part, 0, cy, :, :rows]
                else:
                    g_ref[:, cx, span, :] = s5[part, 1, cx, :, :rows]
            fifth.append((copies, start_x + done, start_y + done, count))
            done += count

    def cells(start, count):
        for o in range(start, start + count, 2):
            values = inverse_z(g_ref[:, :, 4 * o:4 * o + 8, :].reshape(128, 128), iz_ref[...])
            for k in range(2):
                scale = [
                    jnp.concatenate([local_ref[o + k:o + k + 1, 128 * j:128 * j + 128]] * 2, 1)
                    for j in range(4)
                ]
                for x in range(8):
                    cell = slice(16 * x, 16 * x + 16)
                    value = values[cell, 256 * k:256 * k + 256] + scale[3]
                    for j in range(3):
                        value += scale[j] * adv_ref[j, cell, :]
                    out_ref[o + k, x] = activate(value).astype(BF16)

    for piece, (start, count) in enumerate(PIECES):
        for copy in fourth[piece]:
            copy.wait_recv()
        cells(start, count)
    for copies in [first, second] + third + meets + fourth:
        for copy in copies:
            copy.wait_send()
    for part, (copies, start_x, start_y, count) in enumerate(fifth):
        if part:
            for copy in fifth[part - 1][0]:
                copy.wait_send()
        for copy in copies:
            copy.wait_recv()
        cells(start_x, count)
        cells(start_y, count)
    for copy in fifth[-1][0]:
        copy.wait_send()


def per_device(
    velocity, tendency, step_size, lift_weight, lift_bias, spectral_weight, local_weight, local_bias
):
    const = {name: jnp.asarray(a) for name, a in tables().items()}
    far = [
        step_size, velocity.reshape(3, 128, 256), tendency.reshape(3, 128, 256), const["fwd_z"],
        const["by"], const["tw_y"], const["bx"], const["tw_x"], lift_weight.T, lift_bias[None, :],
        local_weight, local_bias[None, :], spectral_weight, const["inv_x"],
        const["ey"], const["tw_i"], const["inv_z"],
    ]
    dma = pltpu.SemaphoreType.DMA
    out = pl.pallas_call(
        layer_kernel,
        out_shape=pltpu.VMEM((32, 8, 16, 256), BF16),
        in_specs=[pl.BlockSpec(memory_space=pl.ANY)] * len(far),
        out_specs=pl.BlockSpec(memory_space=pltpu.VMEM),
        scratch_shapes=[pltpu.SMEM((1,), F32)] + [pltpu.VMEM(a.shape, a.dtype) for a in far[1:]] + [
            pltpu.VMEM((3, 128, 256), F32), pltpu.VMEM((32, 512), F32),
            pltpu.VMEM((256, 128), F32), pltpu.VMEM((16, 16, 128), F32),
            pltpu.VMEM((16, 8, 128), F32), pltpu.VMEM((16, 8, 128), F32),
            pltpu.VMEM((2, 16, 8, 128), F32), pltpu.VMEM((2, 16, 8, 128), F32),
            pltpu.VMEM((16, 64, 128), F32), pltpu.VMEM((2, 4, 64, 256), F32),
            pltpu.VMEM((4, 2, 4, 4, 16, 128), F32), pltpu.VMEM((4, 4, 128, 128), F32),
            pltpu.VMEM((8, 32), F32), pltpu.VMEM((2, 2, 4, 32, 128), F32),
            dma((len(far),)), dma((N,)), dma((N,)), dma((N,)), dma((N,)),
            dma((2, N)), dma((2, N)), dma((len(PIECES), N)), dma((len(PIECES), N)),
            dma((2, 2, 4)), dma((2, 2, 4)), dma((4, 2, 4)), dma((4, 2, 4)),
        ],
        compiler_params=pltpu.CompilerParams(
            collective_id=0, has_side_effects=True, vmem_limit_bytes=VMEM_LIMIT),
        name="layer",
    )(*far)
    return out.reshape(1, 32, 8, 16, 256)


def solution(mesh):
    in_specs = (
        P(None, None, "row", "col", None),
        P(None, None, "row", "col", None),
        P(),
        P(),
        P(),
        P(None, "row", "col", None, None),
        P(),
        P(),
    )
    out_specs = P(None, None, "row", "col", None)
    return jax.shard_map(
        per_device, mesh=mesh, in_specs=in_specs, out_specs=out_specs, check_vma=False
    )
```
